32 devices in a mesh: seq: 8 (over z, y), grp: 4 (over x, core).
Axes of the slice: x: 2, y: 2, z: 4, core: 2. Of those that a mesh axis runs over, the one named last changes fastest.
Arguments:
- hidden: bfloat16 [4096, 2048], P('seq', 'grp'), may hold values from -8 to 8
- qkv_weight: bfloat16 [3, 2048, 6144], P(None, 'seq', 'grp'), may hold values from -0.125 to 0.125
- out_weight: bfloat16 [3, 2048, 2048], P(None, 'grp', 'seq'), may hold values from -0.125 to 0.125
- projection: float32 [3, 16, 128, 128], P(None, 'grp'), may hold values from -6 to 6
- norm_gain: float32 [3, 2048], replicated, may hold values from 0.1 to 1.9
- out_gain: float32 [3, 2048], P(None, 'grp'), may hold values from 0.1 to 1.9
Outputs:
- layer_out: bfloat16 [4096, 2048], P('seq', 'grp')
The draws below stay inside these ranges and needn't reach their ends.
All inputs are finite; a program needn't handle non-finite values.
Results may differ from the reference program's by a relative error of at most 0.034.
Values may be sent and summed in bfloat16 or wider, within the bound.
A program may use at most 64 MiB of HBM per device.

```python
import math
import jax
import jax.numpy as jnp
from jax import lax

D = 2048
H = 16
E = 128
M = 128
LAYERS = 3
TOK_DEV = 512
TOKENS = 4096
N_GRP = 4


def draw_hidden(key, part):
    base = jax.random.normal(jax.random.fold_in(key, 11), (TOKENS, D), jnp.float32)
    return jnp.clip(base, -8.0, 8.0).astype(jnp.bfloat16)


def block_scale(key, extent, shards, least, high):
    gain = 1.0
    for position, blocks in shards:
        heights = jax.random.uniform(jax.random.fold_in(jax.random.fold_in(key, 6), position), (blocks,), jnp.float32, least / len(shards), high / len(shards))
        gain = gain * jnp.repeat(jnp.exp(heights), extent[position] // blocks).reshape((-1,) + (1,) * (len(extent) - 1 - position))
    return gain


def normal_values(key, shape, scale, limit, pieces=(), held_as=jnp.bfloat16):
    gain = block_scale(key, shape, pieces, -0.22, 0.18) if pieces else 1.0
    drawn = jax.random.normal(key, shape, jnp.float32) * scale * gain
    return jnp.minimum(jnp.maximum(drawn, -limit), limit).astype(held_as)


def setup_inputs(seed: int = 0) -> dict:
    splits = jax.random.split(jax.random.key(seed), 7)
    hidden = draw_hidden(jax.random.fold_in(splits[6], 71), 0)
    qkv_weight = normal_values(splits[1], (LAYERS, D, 3 * H * E), D ** -0.5, 0.125, ((1, 8), (2, 4)))
    out_weight = normal_values(splits[2], (LAYERS, H * E, D), (H * E) ** -0.5, 0.125, ((1, 4), (2, 8)))
    projection = normal_values(splits[3], (LAYERS, H, E, M), 1.0, 6.0, ((1, 4),), jnp.float32)
    norm_gain = jnp.clip(1.0 + 0.18 * jax.random.normal(splits[4], (LAYERS, D), jnp.float32), 0.1, 1.9)
    out_gain = jnp.clip(1.0 + 0.18 * jax.random.normal(splits[5], (LAYERS, H * E), jnp.float32), 0.1, 1.9)
    return {"hidden": hidden, "qkv_weight": qkv_weight, "out_weight": out_weight, "projection": projection, "norm_gain": norm_gain, "out_gain": out_gain}


stabilizer = 2.0
highest = lax.Precision.HIGHEST

def features(rows, projection_layer):
    scaled = rows.astype(jnp.float32) * E ** (-0.25)
    mixed = jnp.einsum('thd,hdm->thm', scaled, projection_layer, precision=highest)
    energy = 0.5 * lax.optimization_barrier(jnp.sum(scaled * scaled, axis=-1, keepdims=True))
    return (jnp.exp(mixed - energy - stabilizer) / math.sqrt(M)).astype(jnp.bfloat16)

def block_step(carried, block):
    prefix_kv, prefix_z = carried
    query_feat, key_feat, value_rows = block
    query_wide = query_feat.astype(jnp.float32)
    key_wide = key_feat.astype(jnp.float32)
    value_wide = value_rows.astype(jnp.float32)
    scores = jnp.einsum('ihm,jhm->hij', query_wide, key_wide, precision=highest)
    count = scores.shape[-1]
    causal_mask = jnp.arange(count)[:, None] >= jnp.arange(count)[None, :]
    masked = jnp.where(causal_mask[None], scores, jnp.zeros_like(scores))
    score_weights = lax.optimization_barrier(masked.astype(jnp.bfloat16)).astype(jnp.float32)
    rounded_kv = lax.optimization_barrier(prefix_kv.astype(jnp.bfloat16)).astype(jnp.float32)
    denominator = lax.optimization_barrier(jnp.sum(masked, axis=-1)) + jnp.einsum('ihm,hm->hi', query_wide, prefix_z, precision=highest)
    numerator = jnp.einsum('hij,jhe->hie', score_weights, value_wide, precision=highest)
    numerator = numerator + jnp.einsum('ihm,hme->hie', query_wide, rounded_kv, precision=highest)
    attention = numerator / denominator[..., None]
    block_kv = jnp.einsum('jhm,jhe->hme', key_wide, value_wide, precision=highest)
    block_z = lax.optimization_barrier(jnp.sum(key_wide, axis=0))
    return ((prefix_kv + block_kv, prefix_z + block_z), jnp.transpose(attention, (1, 0, 2)))

def reference(hidden, qkv_weight, out_weight, projection, norm_gain, out_gain):
    stream = hidden
    blocks = TOKENS // TOK_DEV
    group_cols = H // N_GRP * E
    for layer_index in range(LAYERS):
        wide = stream.astype(jnp.float32)
        inverse_rms = lax.rsqrt(lax.optimization_barrier(jnp.mean(wide * wide, axis=-1, keepdims=True)) + 1e-05)
        normed = (wide * inverse_rms * norm_gain[layer_index][None, :]).astype(jnp.bfloat16)
        qkv = jnp.dot(normed, qkv_weight[layer_index], preferred_element_type=jnp.float32).astype(jnp.bfloat16)
        qkv = qkv.reshape(TOKENS, H, 3, E)
        query_feat = features(qkv[:, :, 0], projection[layer_index])
        key_feat = features(qkv[:, :, 1], projection[layer_index])
        value_rows = qkv[:, :, 2]
        start_state = (jnp.zeros((H, M, E), jnp.float32), jnp.zeros((H, M), jnp.float32))
        packed = (query_feat.reshape(blocks, TOK_DEV, H, M), key_feat.reshape(blocks, TOK_DEV, H, M), value_rows.reshape(blocks, TOK_DEV, H, E))
        final_state, attention = lax.scan(block_step, start_state, packed)
        attention = attention.reshape(TOKENS, H, E)
        inverse_norm = lax.rsqrt(lax.optimization_barrier(jnp.mean(attention * attention, axis=-1, keepdims=True)) + 1e-06)
        attended = (attention * inverse_norm * out_gain[layer_index].reshape(H, E)[None]).astype(jnp.bfloat16)
        attended = attended.reshape(TOKENS, H * E)
        summed = jnp.zeros((TOKENS, D), jnp.float32)
        for group_index in range(N_GRP):
            lower = group_index * group_cols
            partial_value = jnp.dot(attended[:, lower:lower + group_cols], out_weight[layer_index][lower:lower + group_cols], preferred_element_type=jnp.float32)
            summed = summed + lax.optimization_barrier(partial_value.astype(jnp.bfloat16)).astype(jnp.float32)
        stream = (stream.astype(jnp.float32) + summed).astype(jnp.bfloat16)
    return stream
```

```python
import functools
import math

import jax
import jax.numpy as jnp
from jax import lax
from jax.experimental import pallas as pl
from jax.experimental.pallas import tpu as pltpu
from jax.sharding import PartitionSpec as P

MESH = pl.DeviceIdType.MESH
stabilizer = 2.0
f32 = jnp.float32
bf16 = jnp.bfloat16


def remote(src, dst, send, recv, device):
    return pltpu.make_async_remote_copy(
        src_ref=src, dst_ref=dst, send_sem=send, recv_sem=recv, device_id=device, device_id_type=MESH
    )


def kernel(
    n_seq, n_grp, hidden, qkv_w, out_w, proj, norm_gain, out_gain, out,
    wq, wo, xg, part, rsd, rx, ry, rv, ru, ub, vb, normed, qf, kf, vf, num, den, att,
    own_state, st_send, st_line, prefix,
    local_sem, z_send, z_recv, r_send, y_send, y_recv, l_send, l_recv,
    ag_send, ag_recv, d_send, d_recv, x_send, x_recv, w_send, w_recv, u_send, u_recv, v_send, v_recv,
):
    layers, rows, cols = qkv_w.shape
    depth, oc = out_w.shape[1:]
    tokens, width = hidden.shape
    heads, head = proj.shape[1:3]
    feats = proj.shape[3] // 3
    lines = n_seq // 2
    chips = n_grp // 2
    mine = heads // 2
    half = tokens // 2
    step_rows = 64
    me = lax.axis_index("seq")
    grp = lax.axis_index("grp")
    line, parity = me // 2, me % 2
    other = 1 - parity
    pair = line * 2 + other
    chip, core = grp // 2, grp % 2
    partner = chip * 2 + 1 - core

    def chip_at(j):
        return lax.rem(chip + j, chips)

    def beside(j):
        return chip_at(j) * 2 + core

    def piece(h):
        return pl.ds(h * half, half)

    def weight(l, k, slot):
        return (wo if k else wq).at[l, slot]

    def own_part(l, k, who):
        if k:
            return out_w.at[l, pl.ds(pl.multiple_of(who * (depth // 2), depth // 2), depth // 2)]
        return qkv_w.at[l, :, pl.ds(pl.multiple_of(who * (cols // 2), cols // 2), cols // 2)]

    own_copies = [
        [pltpu.make_async_copy(own_part(l, k, parity), weight(l, k, me), local_sem.at[1 + 2 * l + k]) for k in range(2)]
        for l in range(layers)
    ]
    own_hidden = pltpu.make_async_copy(hidden, xg.at[parity, grp], local_sem.at[0])
    own_hidden.start()
    for both in own_copies:
        for c in both:
            c.start()

    barrier = pltpu.get_barrier_semaphore()
    for k in range(1, lines):
        pl.semaphore_signal(barrier, inc=1, device_id={"seq": lax.rem(line + k, lines) * 2 + parity}, device_id_type=MESH)
    pl.semaphore_signal(barrier, inc=1, device_id={"seq": pair}, device_id_type=MESH)
    for k in range(1, n_grp):
        pl.semaphore_signal(barrier, inc=1, device_id={"grp": lax.rem(grp + k, n_grp)}, device_id_type=MESH)
    pl.semaphore_wait(barrier, lines + n_grp - 1)

    reach = max(1, lines - 2)
    relays = ((lines - 2, 0, lines - 1), (1, lines - 1, 0)) if lines > 2 else ()

    def slot_of(where, side):
        return where * 2 + (other if side else parity)

    def y_copy(l, k):
        return remote(own_part(l, k, other), weight(l, k, me), y_send.at[l, k], y_recv.at[l, k], {"seq": pair})

    def y_arrival(l, k):
        return remote(weight(l, k, pair), weight(l, k, pair), y_send.at[l, k], y_recv.at[l, k], {"seq": pair})

    def z_copy(l, k, side, to):
        ref = weight(l, k, slot_of(line, side))
        return remote(ref, ref, z_send.at[l, k, side, to], z_recv.at[l, k, slot_of(line, side)], {"seq": to * 2 + parity})

    def z_arrival(l, k, side, src):
        ref = weight(l, k, slot_of(src, side))
        return remote(ref, ref, z_send.at[l, k, side, src], z_recv.at[l, k, slot_of(src, side)], {"seq": pair})

    def r_copy(l, k, side, way):
        _, src, to = relays[way]
        ref = weight(l, k, slot_of(src, side))
        return remote(ref, ref, r_send.at[l, k, side, way], z_recv.at[l, k, slot_of(src, side)], {"seq": to * 2 + parity})

    def span(count, body):
        if count <= 4:
            for t in range(count):
                body(t)
        else:
            pl.loop(0, count)(body)

    def z_each(l, k, side, act):
        def body(t):
            d = reach - t

            @pl.when(line + d < lines)
            def _():
                act(z_copy(l, k, side, line + d))

            @pl.when(line >= d)
            def _():
                act(z_copy(l, k, side, line - d))

        if lines > 1:
            span(reach, body)

    def start(c):
        c.start()

    def z_start(l, k, side):
        z_each(l, k, side, start)

    def relay(l, k):
        for way, (where, src, _) in enumerate(relays):
            @pl.when(line == where)
            def _(way=way, src=src):
                for side in range(2):
                    z_arrival(l, k, side, src).wait_recv()
                    r_copy(l, k, side, way).start()

    def weights_wait(l, k):
        def body(src):
            due = src != line
            for where, taken, _ in relays:
                due = due & jnp.logical_not((line == where) & (src == taken))

            @pl.when(due)
            def _():
                for side in range(2):
                    z_arrival(l, k, side, src).wait_recv()

        span(lines, body)

    def send_next(l):
        for c in own_copies[l]:
            c.wait()
        for k in range(2):
            y_arrival(l, k).wait_recv()
        for k in range(2):
            for side in range(2):
                z_start(l, k, side)

    def ag_copy(l, p, g, h, kind, device):
        ref = xg.at[p, g, piece(h)]
        return remote(ref, ref, ag_send.at[p, g, h, kind], ag_recv.at[l, p, g, h], device)

    to_pair, to_partner = {"seq": pair}, {"grp": partner}

    def ag_wait(l, p, g, h):
        ag_copy(l, p, g, h, 0, to_pair).wait_recv()

    def ag_sends(l):
        first, second = [], []
        for j in range(1, chips):
            first.append((parity, grp, 1, 1 + j, {"grp": beside(j)}))
        first.append((parity, grp, 0, 1, to_pair))
        for j in range(1, chips):
            first.append((parity, grp, 0, 1 + j, {"grp": beside(j)}))
        first.append((parity, grp, 1, 1, to_pair))
        for h in range(2):
            first.append((parity, grp, h, 0, to_partner))
        forward = [((other, grp, 0), [(1 + j, {"grp": beside(j)}) for j in range(1, chips)])]
        for j in range(1, chips):
            forward.append(((parity, beside(j), 1), [(1, to_pair)]))
        forward.append(((other, grp, 1), []))
        for j in range(1, chips):
            forward.append(((parity, beside(j), 0), []))
        for j in range(1, chips):
            for h in range(2):
                forward.append(((other, beside(j), h), []))
        for slot, targets in forward:
            second.append((slot, [slot + t for t in targets + [(0, to_partner)]]))
        return first, second

    def ag_start(l):
        for args in ag_sends(l)[0]:
            ag_copy(l, *args).start()

    def ag_finish(l):
        first, second = ag_sends(l)
        for slot, targets in second:
            ag_wait(l, *slot)
            for args in targets:
                ag_copy(l, *args).start()
        for h in range(2):
            for p in (parity, other):
                ag_wait(l, p, partner, h)
                for j in range(1, chips):
                    ag_wait(l, p, chip_at(j) * 2 + 1 - core, h)

    def ag_drain(l):
        first, second = ag_sends(l)
        for args in first + [a for _, targets in second for a in targets]:
            ag_copy(l, *args).wait_send()

    def d_copy(l, p, x):
        return remote(part.at[p, x * 2 + 1 - core], rsd.at[p, x], d_send.at[p, x], d_recv.at[l, p, x], to_partner)

    def x_copy(l, p, j):
        return remote(
            part.at[p, beside(j), piece(0)], rx.at[p, chip], x_send.at[p, j], x_recv.at[l, p, chip], {"grp": beside(j)}
        )

    def x_arrival(l, p, j):
        ref = rx.at[p, chip_at(j)]
        return remote(ref, ref, x_send.at[p, j], x_recv.at[l, p, chip_at(j)], {"grp": beside(j)})

    def w_copy(l, j):
        x = chip_at(j)
        return remote(part.at[other, beside(j), piece(1)], ry.at[x], w_send.at[x], w_recv.at[l, x], to_pair)

    def u_copy(l):
        return remote(ub, ru, u_send.at[0], u_recv.at[l], to_pair)

    def v_copy(l, j):
        return remote(vb.at[chip_at(j)], rv.at[chip], v_send.at[j], v_recv.at[l, chip], {"grp": beside(j)})

    def v_arrival(l, j):
        ref = rv.at[chip_at(j)]
        return remote(ref, ref, v_send.at[j], v_recv.at[l, chip_at(j)], {"grp": beside(j)})

    def line_copy(l, step):
        return remote(
            st_send.at[l], st_line.at[l, line], l_send.at[l, step], l_recv.at[l, line], {"seq": (line + step) * 2 + parity}
        )

    def line_arrival(l, step):
        src = line - step
        return remote(st_send.at[l], st_line.at[l, src], l_send.at[l, step], l_recv.at[l, src], {"seq": src * 2 + parity})

    for k in range(2):
        y_copy(0, k).start()
    for c in own_copies[0]:
        c.wait()
    z_start(0, 0, 0)
    own_hidden.wait()
    ag_start(0)
    y_arrival(0, 0).wait_recv()
    z_start(0, 0, 1)
    z_start(0, 1, 0)
    y_arrival(0, 1).wait_recv()
    z_start(0, 1, 1)

    scale = head ** (-0.25)
    inv = 1.0 / math.sqrt(feats)

    def features(u, terms):
        mixed = jnp.dot(u, terms, preferred_element_type=f32)
        mixed = (mixed[:, 2 * feats :] + mixed[:, feats : 2 * feats]) + mixed[:, :feats]
        w0 = u.astype(f32) * scale
        energy = 0.5 * jnp.sum(w0 * w0, axis=-1, keepdims=True)
        return (jnp.exp(mixed - energy - stabilizer) * inv).astype(bf16)

    for l in range(layers):
        last = l == layers - 1
        ag_finish(l)
        if l == 0:
            for n in range(1, layers):
                for k in range(2):
                    y_copy(n, k).start()

        @pl.loop(0, 2 * tokens // step_rows)
        def _(t):
            at = pl.ds(pl.multiple_of(t * step_rows, step_rows), step_rows)
            b = t // (tokens // step_rows)
            src = pl.ds(pl.multiple_of(t % (tokens // step_rows) * step_rows, step_rows), step_rows)
            wide = [xg[b, g, src, :].astype(f32) for g in range(n_grp)]
            total = sum(jnp.sum(v * v, axis=-1, keepdims=True) for v in wide)
            rms = lax.rsqrt(total / (width * n_grp) + 1e-05)
            for g in range(n_grp):
                cut = slice(g * width, (g + 1) * width)
                normed[at, cut] = (wide[g] * rms * norm_gain[l : l + 1, cut]).astype(bf16)

        ag_drain(l)
        relay(l, 0)
        middle = 0 < l < layers - 1
        if middle:
            relay(l, 1)
            send_next(l + 1)
        weights_wait(l, 0)

        @pl.loop(0, 2 * mine)
        def _(i):
            h, b = i // 2, i % 2
            at = pl.ds(pl.multiple_of(h * 3 * head, 128), 3 * head)
            w = wq[l, :, :, at].reshape(n_seq * rows, 3 * head)
            x = normed[pl.ds(pl.multiple_of(b * tokens, tokens), tokens), :]
            qkv = jnp.dot(x, w, preferred_element_type=f32).astype(bf16)
            terms = proj[l, parity * mine + h]
            key = features(qkv[:, head : 2 * head], terms)
            value = qkv[:, 2 * head :]
            qf[i] = features(qkv[:, :head], terms)
            kf[i] = key
            vf[i] = value
            own_state[i, :feats] = lax.dot_general(key, value, (((0,), (0,)), ((), ())), preferred_element_type=f32)
            own_state[i, feats:] = jnp.dot(jnp.ones((16, tokens), bf16), key, preferred_element_type=f32)

        for h in range(mine):
            st_send[l, h] = (own_state[2 * h] + own_state[2 * h + 1]).astype(bf16)

        def send_state(t):
            @pl.when(line + t + 1 < lines)
            def _():
                line_copy(l, t + 1).start()

        span(lines - 1, send_state)
        if not middle:
            relay(l, 1)
            if not last:
                send_next(l + 1)

        @pl.loop(0, 2 * mine)
        def _(i):
            scores = lax.dot_general(qf[i], kf[i], (((1,), (1,)), ((), ())), preferred_element_type=f32)
            r = lax.broadcasted_iota(jnp.int32, (tokens, tokens), 0)
            c = lax.broadcasted_iota(jnp.int32, (tokens, tokens), 1)
            masked = jnp.where(r >= c, scores, 0.0)
            den[i] = jnp.broadcast_to(jnp.sum(masked, axis=-1, keepdims=True), (tokens, head))
            num[i] = jnp.dot(masked.astype(bf16), vf[i], preferred_element_type=f32)

        for h in range(mine):
            prefix[h] = jnp.zeros_like(prefix[h])

        def take_state(t):
            step = t + 1

            @pl.when(line >= step)
            def _():
                line_arrival(l, step).wait_recv()
                for h in range(mine):
                    prefix[h] = prefix[h] + st_line[l, line - step, h].astype(f32)

        span(lines - 1, take_state)

        @pl.loop(0, 2 * mine)
        def _(i):
            h, b = i // 2, i % 2
            before = prefix[h] + own_state[2 * h] * jnp.where(b == 1, 1.0, 0.0)
            q = qf[i]
            d = den[i] + jnp.sum(q.astype(f32) * before[feats : feats + 1], axis=-1, keepdims=True)
            n = num[i] + jnp.dot(q, before[:feats].astype(bf16), preferred_element_type=f32)
            a = n / d
            norm = lax.rsqrt(jnp.mean(a * a, axis=-1, keepdims=True) + 1e-06)
            to_rows = pl.ds(pl.multiple_of(b * tokens, tokens), tokens)
            to_cols = pl.ds(pl.multiple_of(h * head, 128), head)
            att[to_rows, to_cols] = (a * norm * out_gain[l, parity * mine + h]).astype(bf16)

        weights_wait(l, 1)
        per = width // oc

        def project(p, g):
            a = att[pl.ds(pl.multiple_of(p * tokens, tokens), tokens), :]
            for i in range(per):
                part[p, g, :, i * oc : (i + 1) * oc] = jnp.dot(
                    a, wo[l, g * per + i], preferred_element_type=f32
                ).astype(bf16)

        @pl.loop(0, 2 * chips)
        def _(n):
            p = lax.rem(other + n // chips, 2)
            x = lax.rem(chip + 1 + n % chips, chips)
            project(p, x * 2 + 1 - core)
            d_copy(l, p, x).start()

        @pl.loop(0, 2 * chips)
        def _(n):
            p = lax.rem(other + n // chips, 2)
            x = lax.rem(chip + 1 + n % chips, chips)
            project(p, x * 2 + core)

        hops = list(range(1, chips)) + [0]
        for own in range(2):
            p = parity if own else other
            for j in hops:
                x = chip_at(j)
                d_copy(l, p, x).wait_recv()

                @pl.loop(0, tokens // step_rows)
                def _(t, p=p, x=x, j=j):
                    at = pl.ds(pl.multiple_of(t * step_rows, step_rows), step_rows)
                    part[p, beside(j), at, :] = (
                        part[p, beside(j), at, :].astype(f32) + rsd[p, x, at, :].astype(f32)
                    ).astype(bf16)

                if j:
                    x_copy(l, p, j).start()
                if not own:
                    w_copy(l, j).start()

        for j in range(1, chips):
            x_arrival(l, other, j).wait_recv()

        @pl.loop(0, half // step_rows)
        def _(t):
            at = pl.ds(pl.multiple_of(t * step_rows, step_rows), step_rows)
            total = part[other, grp, at, :].astype(f32)
            for j in range(1, chips):
                total = total + rx[other, chip_at(j), at, :].astype(f32)
            ub[at, :] = total.astype(bf16)

        u_copy(l).start()
        for j in hops:
            w_arrival = remote(ry.at[chip_at(j)], ry.at[chip_at(j)], w_send.at[j], w_recv.at[l, chip_at(j)], to_pair)
            w_arrival.wait_recv()
            if j:
                @pl.loop(0, half // step_rows)
                def _(t, j=j):
                    at = pl.ds(pl.multiple_of(t * step_rows, step_rows), step_rows)
                    low = pl.ds(pl.multiple_of(half + t * step_rows, step_rows), step_rows)
                    vb[chip_at(j), at, :] = (
                        part[parity, beside(j), low, :].astype(f32) + ry[chip_at(j), at, :].astype(f32)
                    ).astype(bf16)

                v_copy(l, j).start()
        for j in range(1, chips):
            x_arrival(l, parity, j).wait_recv()
        u_copy(l).wait_recv()

        def finish(at, total):
            total = (xg[parity, grp, at, :].astype(f32) + total).astype(bf16)
            if last:
                out[at, :] = total
            else:
                xg[parity, grp, at, :] = total

        @pl.loop(0, half // step_rows)
        def _(t):
            at = pl.ds(pl.multiple_of(t * step_rows, step_rows), step_rows)
            total = part[parity, grp, at, :].astype(f32) + ru[at, :].astype(f32)
            for j in range(1, chips):
                total = total + rx[parity, chip_at(j), at, :].astype(f32)
            finish(at, total)

        for j in range(1, chips):
            v_arrival(l, j).wait_recv()

        @pl.loop(0, half // step_rows)
        def _(t):
            at = pl.ds(pl.multiple_of(t * step_rows, step_rows), step_rows)
            low = pl.ds(pl.multiple_of(half + t * step_rows, step_rows), step_rows)
            total = part[parity, grp, low, :].astype(f32) + ry[chip, at, :].astype(f32)
            for j in range(1, chips):
                total = total + rv[chip_at(j), at, :].astype(f32)
            finish(low, total)

        if not last:
            ag_start(l + 1)
        for p in range(2):
            for x in range(chips):
                d_copy(l, p, x).wait_send()
            for j in range(1, chips):
                x_copy(l, p, j).wait_send()
        for j in range(chips):
            w_copy(l, j).wait_send()
        u_copy(l).wait_send()
        for j in range(1, chips):
            v_copy(l, j).wait_send()

    def wait_send(c):
        c.wait_send()

    for l in range(layers):
        for k in range(2):
            y_copy(l, k).wait_send()
            for side in range(2):
                z_each(l, k, side, wait_send)
            for way, (where, _, _) in enumerate(relays):
                @pl.when(line == where)
                def _(way=way):
                    for side in range(2):
                        r_copy(l, k, side, way).wait_send()

        def state_sent(t):
            @pl.when(line + t + 1 < lines)
            def _():
                line_copy(l, t + 1).wait_send()

        span(lines - 1, state_sent)


def local(n_seq, n_grp, hidden, qkv_weight, out_weight, projection, norm_gain, out_gain):
    layers, rows, cols = qkv_weight.shape
    depth, oc = out_weight.shape[1:]
    heads, head, feats = projection.shape[1:]
    tokens, width = hidden.shape
    lines, chips, mine, half = n_seq // 2, n_grp // 2, heads // 2, tokens // 2
    scaled = projection * head ** (-0.25)
    high = lax.reduce_precision(scaled, 8, 7)
    rest = scaled - high
    mid = lax.reduce_precision(rest, 8, 7)
    low = rest - mid
    terms = jnp.concatenate([high, mid, low], axis=-1).astype(bf16)
    gains = out_gain.reshape(layers, heads, 1, head)
    dma = pltpu.SemaphoreType.DMA
    vmem = pl.BlockSpec(memory_space=pltpu.VMEM)
    anywhere = pl.BlockSpec(memory_space=pl.ANY)
    state = (feats + 16, head)
    return pl.pallas_call(
        functools.partial(kernel, n_seq, n_grp),
        out_shape=jax.ShapeDtypeStruct((tokens, width), bf16),
        in_specs=[anywhere, anywhere, anywhere, vmem, vmem, vmem],
        out_specs=vmem,
        scratch_shapes=[
            pltpu.VMEM((layers, n_seq, rows, cols // 2), bf16),
            pltpu.VMEM((layers, n_seq, depth // 2, oc), bf16),
            pltpu.VMEM((2, n_grp, tokens, width), bf16),
            pltpu.VMEM((2, n_grp, tokens, width), bf16),
            pltpu.VMEM((2, chips, tokens, width), bf16),
            pltpu.VMEM((2, chips, half, width), bf16),
            pltpu.VMEM((chips, half, width), bf16),
            pltpu.VMEM((chips, half, width), bf16),
            pltpu.VMEM((half, width), bf16),
            pltpu.VMEM((half, width), bf16),
            pltpu.VMEM((chips, half, width), bf16),
            pltpu.VMEM((2 * tokens, n_grp * width), bf16),
            pltpu.VMEM((heads, tokens, feats), bf16),
            pltpu.VMEM((heads, tokens, feats), bf16),
            pltpu.VMEM((heads, tokens, head), bf16),
            pltpu.VMEM((heads, tokens, head), f32),
            pltpu.VMEM((heads, tokens, head), f32),
            pltpu.VMEM((2 * tokens, mine * head), bf16),
            pltpu.VMEM((heads,) + state, f32),
            pltpu.VMEM((layers, mine) + state, bf16),
            pltpu.VMEM((layers, lines, mine) + state, bf16),
            pltpu.VMEM((mine,) + state, f32),
            dma((1 + 2 * layers,)),
            dma((layers, 2, 2, lines)),
            dma((layers, 2, n_seq)),
            dma((layers, 2, 2, 2)),
            dma((layers, 2)),
            dma((layers, 2)),
            dma((layers, lines)),
            dma((layers, lines)),
            dma((2, n_grp, 2, 1 + chips)),
            dma((layers, 2, n_grp, 2)),
            dma((2, chips)),
            dma((layers, 2, chips)),
            dma((2, chips)),
            dma((layers, 2, chips)),
            dma((chips,)),
            dma((layers, chips)),
            dma((1,)),
            dma((layers,)),
            dma((chips,)),
            dma((layers, chips)),
        ],
        compiler_params=pltpu.CompilerParams(
            collective_id=0, has_side_effects=True, vmem_limit_bytes=66_000_000
        ),
    )(hidden, qkv_weight, out_weight, terms, norm_gain, gains)


def solution(mesh):
    return jax.shard_map(
        functools.partial(local, mesh.shape["seq"], mesh.shape["grp"]),
        mesh=mesh,
        in_specs=(
            P("seq", "grp"),
            P(None, "seq", "grp"),
            P(None, "grp", "seq"),
            P(None, "grp", None, None),
            P(),
            P(None, "grp"),
        ),
        out_specs=P("seq", "grp"),
        check_vma=False,
    )
```

```python
import functools
import math

import jax
import jax.numpy as jnp
from jax import lax
from jax.experimental import pallas as pl
from jax.experimental.pallas import tpu as pltpu
from jax.sharding import PartitionSpec as P

MESH = pl.DeviceIdType.MESH
stabilizer = 2.0
f32 = jnp.float32
bf16 = jnp.bfloat16


def remote(src, dst, send, recv, device):
    return pltpu.make_async_remote_copy(
        src_ref=src, dst_ref=dst, send_sem=send, recv_sem=recv, device_id=device, device_id_type=MESH
    )


def kernel(
    n_seq, n_grp, hidden, qkv_w, out_w, proj, norm_gain, out_gain, out,
    wq, wo, sq, so, xg, part, rsd, rx, ry, rv, ru, ub, vb, normed, qf, kf, vf, num, den, att,
    own_state, st_send, st_held, st_line, prefix,
    local_sem, z_send, s_send, z_recv, r_send, y_send, y_recv, h_send, h_recv, l_send, m_send, l_recv, k_send, k_recv,
    ag_send, ag_recv, d_send, d_recv, x_send, x_recv, w_send, w_recv, u_send, u_recv, v_send, v_recv,
):
    layers, rows, cols = qkv_w.shape
    depth, oc = out_w.shape[1:]
    tokens, width = hidden.shape
    heads, head = proj.shape[1:3]
    feats = proj.shape[3] // 3
    lines = n_seq // 2
    chips = n_grp // 2
    mine = heads // 2
    half = tokens // 2
    step_rows = 64
    me = lax.axis_index("seq")
    grp = lax.axis_index("grp")
    line, parity = me // 2, me % 2
    other = 1 - parity
    pair = line * 2 + other
    chip, core = grp // 2, grp % 2
    partner = chip * 2 + 1 - core

    def chip_at(j):
        return lax.rem(chip + j, chips)

    def beside(j):
        return chip_at(j) * 2 + core

    def piece(h):
        return pl.ds(h * half, half)

    def weight(l, k, slot):
        return (wo if k else wq).at[l, slot]

    def own_part(l, k, who):
        if k:
            return out_w.at[l, pl.ds(pl.multiple_of(who * (depth // 2), depth // 2), depth // 2)]
        return qkv_w.at[l, :, pl.ds(pl.multiple_of(who * (cols // 2), cols // 2), cols // 2)]

    own_copies = [
        [pltpu.make_async_copy(own_part(l, k, parity), weight(l, k, me), local_sem.at[1 + 2 * l + k]) for k in range(2)]
        for l in range(layers)
    ]
    own_hidden = pltpu.make_async_copy(hidden, xg.at[parity, grp], local_sem.at[0])
    own_hidden.start()
    for both in own_copies:
        for c in both:
            c.start()

    barrier = pltpu.get_barrier_semaphore()
    for k in range(1, lines):
        along = lax.rem(line + k, lines) * 2 + parity
        pl.semaphore_signal(barrier, inc=1, device_id={"seq": along}, device_id_type=MESH)
        pl.semaphore_signal(barrier, inc=1, device_id={"seq": along, "grp": partner}, device_id_type=MESH)
    pl.semaphore_signal(barrier, inc=1, device_id={"seq": pair}, device_id_type=MESH)
    for k in range(1, n_grp):
        pl.semaphore_signal(barrier, inc=1, device_id={"grp": lax.rem(grp + k, n_grp)}, device_id_type=MESH)
    pl.semaphore_wait(barrier, 2 * lines + n_grp - 2)

    reach = max(1, lines - 2)
    relays = ((lines - 2, 0, lines - 1), (1, lines - 1, 0)) if lines > 2 else ()

    def slot_of(where, side):
        return where * 2 + (other if side else parity)

    def y_copy(l, k):
        return remote(own_part(l, k, other), weight(l, k, me), y_send.at[l, k], y_recv.at[l, k], {"seq": pair})

    def y_arrival(l, k):
        return remote(weight(l, k, pair), weight(l, k, pair), y_send.at[l, k], y_recv.at[l, k], {"seq": pair})

    def z_copy(l, k, side, to):
        ref = weight(l, k, slot_of(line, side))
        return remote(ref, ref, z_send.at[l, k, side, to], z_recv.at[l, k, slot_of(line, side)], {"seq": to * 2 + parity})

    def z_arrival(l, k, side, src):
        ref = weight(l, k, slot_of(src, side))
        return remote(ref, ref, z_send.at[l, k, side, src], z_recv.at[l, k, slot_of(src, side)], {"seq": pair})

    def r_copy(l, k, side, way):
        _, src, to = relays[way]
        ref = weight(l, k, slot_of(src, side))
        return remote(ref, ref, r_send.at[l, k, side, way], z_recv.at[l, k, slot_of(src, side)], {"seq": to * 2 + parity})

    def span(count, body):
        if count <= 4:
            for t in range(count):
                body(t)
        else:
            pl.loop(0, count)(body)

    def held(l, k, side):
        return (so if k else sq).at[l, side]

    def h_copy(l, k, side):
        src = weight(l, k, pair) if side else own_part(l, k, parity)
        return remote(src, held(l, k, side), h_send.at[l, k, side], h_recv.at[l, k, side], {"grp": partner})

    def s_copy(l, k, side, to):
        slot = slot_of(line, side)
        return remote(
            held(l, k, side), weight(l, k, slot), s_send.at[l, k, side, to], z_recv.at[l, k, slot],
            {"seq": to * 2 + parity, "grp": partner},
        )

    def z_each(l, pieces, act):
        def body(t):
            d = reach - t
            for k, side in pieces:
                @pl.when((line + d < lines) & (core == 0))
                def _(k=k, side=side):
                    act(z_copy(l, k, side, line + d))
                    act(s_copy(l, k, side, line + d))

                @pl.when(line >= d)
                def _(k=k, side=side):
                    act(z_copy(l, k, side, line - d))

        if lines > 1:
            span(reach, body)

    def start(c):
        c.start()

    def hand_over(l, k, side):
        @pl.when(core == 1)
        def _():
            h_copy(l, k, side).start()

    def take_over(l, k, side):
        @pl.when(core == 0)
        def _():
            h_copy(l, k, side).wait_recv()

    def z_start(l, *pieces):
        z_each(l, pieces, start)

    def relay(l, k, side):
        for way, (where, src, _) in enumerate(relays):
            @pl.when(line == where)
            def _(way=way, src=src):
                z_arrival(l, k, side, src).wait_recv()
                r_copy(l, k, side, way).start()

    def weights_wait(l, k):
        def body(src):
            due = src != line
            for where, taken, _ in relays:
                due = due & jnp.logical_not((line == where) & (src == taken))

            @pl.when(due)
            def _():
                for side in range(2):
                    z_arrival(l, k, side, src).wait_recv()

        span(lines, body)

    def send_next(l):
        for c in own_copies[l]:
            c.wait()
        for k in range(2):
            for side in range(2):
                take_over(l, k, side)
        if l < layers - 1:
            z_start(l, (0, 0), (0, 1), (1, 0), (1, 1))
        else:
            z_start(l, (0, 0), (0, 1))
            z_start(l, (1, 0), (1, 1))

    def ag_copy(l, p, g, h, kind, device):
        ref = xg.at[p, g, piece(h)]
        return remote(ref, ref, ag_send.at[p, g, h, kind], ag_recv.at[l, p, g, h], device)

    to_pair, to_partner = {"seq": pair}, {"grp": partner}

    def ag_wait(l, p, g, h):
        ag_copy(l, p, g, h, 0, to_pair).wait_recv()

    def ag_sends(l):
        first, second = [], []
        for j in range(1, chips):
            first.append((parity, grp, 1, 1 + j, {"grp": beside(j)}))
        first.append((parity, grp, 0, 1, to_pair))
        for j in range(1, chips):
            first.append((parity, grp, 0, 1 + j, {"grp": beside(j)}))
        first.append((parity, grp, 1, 1, to_pair))
        for h in range(2):
            first.append((parity, grp, h, 0, to_partner))
        forward = [((other, grp, 0), [(1 + j, {"grp": beside(j)}) for j in range(1, chips)])]
        for j in range(1, chips):
            forward.append(((parity, beside(j), 1), [(1, to_pair)]))
        forward.append(((other, grp, 1), []))
        for j in range(1, chips):
            forward.append(((parity, beside(j), 0), []))
        for j in range(1, chips):
            for h in range(2):
                forward.append(((other, beside(j), h), []))
        for slot, targets in forward:
            second.append((slot, [slot + t for t in targets + [(0, to_partner)]]))
        return first, second

    def ag_start(l):
        for args in ag_sends(l)[0]:
            ag_copy(l, *args).start()

    def ag_finish(l):
        first, second = ag_sends(l)
        for slot, targets in second:
            ag_wait(l, *slot)
            for args in targets:
                ag_copy(l, *args).start()
        for h in range(2):
            for p in (parity, other):
                ag_wait(l, p, partner, h)
                for j in range(1, chips):
                    ag_wait(l, p, chip_at(j) * 2 + 1 - core, h)

    def ag_drain(l):
        first, second = ag_sends(l)
        for args in first + [a for _, targets in second for a in targets]:
            ag_copy(l, *args).wait_send()

    def d_copy(l, p, x):
        return remote(part.at[p, x * 2 + 1 - core], rsd.at[p, x], d_send.at[p, x], d_recv.at[l, p, x], to_partner)

    def x_copy(l, p, j):
        return remote(
            part.at[p, beside(j), piece(0)], rx.at[p, chip], x_send.at[p, j], x_recv.at[l, p, chip], {"grp": beside(j)}
        )

    def x_arrival(l, p, j):
        ref = rx.at[p, chip_at(j)]
        return remote(ref, ref, x_send.at[p, j], x_recv.at[l, p, chip_at(j)], {"grp": beside(j)})

    def w_copy(l, j):
        x = chip_at(j)
        return remote(part.at[other, beside(j), piece(1)], ry.at[x], w_send.at[x], w_recv.at[l, x], to_pair)

    def u_copy(l):
        return remote(ub, ru, u_send.at[0], u_recv.at[l], to_pair)

    def v_copy(l, j):
        return remote(vb.at[chip_at(j)], rv.at[chip], v_send.at[j], v_recv.at[l, chip], {"grp": beside(j)})

    def v_arrival(l, j):
        ref = rv.at[chip_at(j)]
        return remote(ref, ref, v_send.at[j], v_recv.at[l, chip_at(j)], {"grp": beside(j)})

    def line_copy(l, step):
        return remote(
            st_send.at[l], st_line.at[l, line], l_send.at[l, step], l_recv.at[l, line], {"seq": (line + step) * 2 + parity}
        )

    def held_copy(l, step):
        return remote(
            st_held.at[l], st_line.at[l, line], m_send.at[l, step], l_recv.at[l, line],
            {"seq": (line + step) * 2 + parity, "grp": partner},
        )

    def state_copy(l):
        return remote(st_send.at[l], st_held.at[l], k_send.at[l], k_recv.at[l], to_partner)

    def line_arrival(l, step):
        src = line - step
        return remote(st_send.at[l], st_line.at[l, src], l_send.at[l, step], l_recv.at[l, src], {"seq": src * 2 + parity})

    for k in range(2):
        y_copy(0, k).start()
    for l in range(layers):
        for k in range(2):
            hand_over(l, k, 0)
    for c in own_copies[0]:
        c.wait()
    take_over(0, 0, 0)
    z_start(0, (0, 0))
    own_hidden.wait()
    ag_start(0)
    for k in range(2):
        y_arrival(0, k).wait_recv()
        hand_over(0, k, 1)
        if k:
            take_over(0, 1, 0)
            z_start(0, (1, 0))
        take_over(0, k, 1)
        z_start(0, (k, 1))
    relay(0, 0, 0)

    scale = head ** (-0.25)
    inv = 1.0 / math.sqrt(feats)

    def features(u, terms):
        mixed = jnp.dot(u, terms, preferred_element_type=f32)
        mixed = (mixed[:, 2 * feats :] + mixed[:, feats : 2 * feats]) + mixed[:, :feats]
        w0 = u.astype(f32) * scale
        energy = 0.5 * jnp.sum(w0 * w0, axis=-1, keepdims=True)
        return (jnp.exp(mixed - energy - stabilizer) * inv).astype(bf16)

    for l in range(layers):
        last = l == layers - 1
        ag_finish(l)
        if l == 0:
            for n in range(1, layers):
                for k in range(2):
                    y_copy(n, k).start()
            relay(0, 0, 1)

        @pl.loop(0, 2 * tokens // step_rows)
        def _(t):
            at = pl.ds(pl.multiple_of(t * step_rows, step_rows), step_rows)
            b = t // (tokens // step_rows)
            src = pl.ds(pl.multiple_of(t % (tokens // step_rows) * step_rows, step_rows), step_rows)
            wide = [xg[b, g, src, :].astype(f32) for g in range(n_grp)]
            total = sum(jnp.sum(v * v, axis=-1, keepdims=True) for v in wide)
            rms = lax.rsqrt(total / (width * n_grp) + 1e-05)
            for g in range(n_grp):
                cut = slice(g * width, (g + 1) * width)
                normed[at, cut] = (wide[g] * rms * norm_gain[l : l + 1, cut]).astype(bf16)

        ag_drain(l)
        if l == 0:
            for n in range(1, layers):
                for k in range(2):
                    y_arrival(n, k).wait_recv()
                    hand_over(n, k, 1)
        middle = 0 < l < layers - 1
        if middle:
            relay(l, 1, 0)
            relay(l, 1, 1)
            send_next(l + 1)
        weights_wait(l, 0)

        @pl.loop(0, 2 * mine)
        def _(i):
            h, b = i // 2, i % 2
            at = pl.ds(pl.multiple_of(h * 3 * head, 128), 3 * head)
            w = wq[l, :, :, at].reshape(n_seq * rows, 3 * head)
            x = normed[pl.ds(pl.multiple_of(b * tokens, tokens), tokens), :]
            qkv = jnp.dot(x, w, preferred_element_type=f32).astype(bf16)
            terms = proj[l, parity * mine + h]
            key = features(qkv[:, head : 2 * head], terms)
            value = qkv[:, 2 * head :]
            qf[i] = features(qkv[:, :head], terms)
            kf[i] = key
            vf[i] = value
            own_state[i, :feats] = lax.dot_general(key, value, (((0,), (0,)), ((), ())), preferred_element_type=f32)
            own_state[i, feats:] = jnp.dot(jnp.ones((16, tokens), bf16), key, preferred_element_type=f32)

        for h in range(mine):
            st_send[l, h] = (own_state[2 * h] + own_state[2 * h + 1]).astype(bf16)

        def send_state(copy):
            def body(t):
                @pl.when((line + t + 1 < lines) & (core == 1))
                def _():
                    copy(l, t + 1).start()

            span(lines - 1, body)

        @pl.when((line + 1 < lines) & (core == 0))
        def _():
            state_copy(l).start()

        send_state(line_copy)

        @pl.when((line + 1 < lines) & (core == 1))
        def _():
            state_copy(l).wait_recv()

        send_state(held_copy)
        if not middle:
            relay(l, 1, 0)
            relay(l, 1, 1)
            if not last:
                send_next(l + 1)

        @pl.loop(0, 2 * mine)
        def _(i):
            scores = lax.dot_general(qf[i], kf[i], (((1,), (1,)), ((), ())), preferred_element_type=f32)
            r = lax.broadcasted_iota(jnp.int32, (tokens, tokens), 0)
            c = lax.broadcasted_iota(jnp.int32, (tokens, tokens), 1)
            masked = jnp.where(r >= c, scores, 0.0)
            den[i] = jnp.broadcast_to(jnp.sum(masked, axis=-1, keepdims=True), (tokens, head))
            num[i] = jnp.dot(masked.astype(bf16), vf[i], preferred_element_type=f32)

        for h in range(mine):
            prefix[h] = jnp.zeros_like(prefix[h])

        def take_state(t):
            step = t + 1

            @pl.when(line >= step)
            def _():
                line_arrival(l, step).wait_recv()
                for h in range(mine):
                    prefix[h] = prefix[h] + st_line[l, line - step, h].astype(f32)

        span(lines - 1, take_state)

        @pl.loop(0, 2 * mine)
        def _(i):
            h, b = i // 2, i % 2
            before = prefix[h] + own_state[2 * h] * jnp.where(b == 1, 1.0, 0.0)
            q = qf[i]
            d = den[i] + jnp.sum(q.astype(f32) * before[feats : feats + 1], axis=-1, keepdims=True)
            n = num[i] + jnp.dot(q, before[:feats].astype(bf16), preferred_element_type=f32)
            a = n / d
            norm = lax.rsqrt(jnp.mean(a * a, axis=-1, keepdims=True) + 1e-06)
            to_rows = pl.ds(pl.multiple_of(b * tokens, tokens), tokens)
            to_cols = pl.ds(pl.multiple_of(h * head, 128), head)
            att[to_rows, to_cols] = (a * norm * out_gain[l, parity * mine + h]).astype(bf16)

        weights_wait(l, 1)
        per = width // oc

        def project(p, g):
            a = att[pl.ds(pl.multiple_of(p * tokens, tokens), tokens), :]
            for i in range(per):
                part[p, g, :, i * oc : (i + 1) * oc] = jnp.dot(
                    a, wo[l, g * per + i], preferred_element_type=f32
                ).astype(bf16)

        @pl.loop(0, 2 * chips)
        def _(n):
            p = lax.rem(other + n // chips, 2)
            x = lax.rem(chip + 1 + n % chips, chips)
            project(p, x * 2 + 1 - core)
            d_copy(l, p, x).start()

        @pl.loop(0, 2 * chips)
        def _(n):
            p = lax.rem(other + n // chips, 2)
            x = lax.rem(chip + 1 + n % chips, chips)
            project(p, x * 2 + core)

        if not last:
            relay(l + 1, 0, 0)
        hops = list(range(1, chips)) + [0]
        for own in range(2):
            p = parity if own else other
            for j in hops:
                x = chip_at(j)
                d_copy(l, p, x).wait_recv()

                @pl.loop(0, tokens // step_rows)
                def _(t, p=p, x=x, j=j):
                    at = pl.ds(pl.multiple_of(t * step_rows, step_rows), step_rows)
                    part[p, beside(j), at, :] = (
                        part[p, beside(j), at, :].astype(f32) + rsd[p, x, at, :].astype(f32)
                    ).astype(bf16)

                if j:
                    x_copy(l, p, j).start()
                if not own:
                    w_copy(l, j).start()

        for j in range(1, chips):
            x_arrival(l, other, j).wait_recv()

        @pl.loop(0, half // step_rows)
        def _(t):
            at = pl.ds(pl.multiple_of(t * step_rows, step_rows), step_rows)
            total = part[other, grp, at, :].astype(f32)
            for j in range(1, chips):
                total = total + rx[other, chip_at(j), at, :].astype(f32)
            ub[at, :] = total.astype(bf16)

        u_copy(l).start()
        for j in hops:
            w_arrival = remote(ry.at[chip_at(j)], ry.at[chip_at(j)], w_send.at[j], w_recv.at[l, chip_at(j)], to_pair)
            w_arrival.wait_recv()
            if j:
                @pl.loop(0, half // step_rows)
                def _(t, j=j):
                    at = pl.ds(pl.multiple_of(t * step_rows, step_rows), step_rows)
                    low = pl.ds(pl.multiple_of(half + t * step_rows, step_rows), step_rows)
                    vb[chip_at(j), at, :] = (
                        part[parity, beside(j), low, :].astype(f32) + ry[chip_at(j), at, :].astype(f32)
                    ).astype(bf16)

                v_copy(l, j).start()
        for j in range(1, chips):
            x_arrival(l, parity, j).wait_recv()
        u_copy(l).wait_recv()

        def finish(at, total):
            total = (xg[parity, grp, at, :].astype(f32) + total).astype(bf16)
            if last:
                out[at, :] = total
            else:
                xg[parity, grp, at, :] = total

        @pl.loop(0, half // step_rows)
        def _(t):
            at = pl.ds(pl.multiple_of(t * step_rows, step_rows), step_rows)
            total = part[parity, grp, at, :].astype(f32) + ru[at, :].astype(f32)
            for j in range(1, chips):
                total = total + rx[parity, chip_at(j), at, :].astype(f32)
            finish(at, total)

        for j in range(1, chips):
            v_arrival(l, j).wait_recv()

        @pl.loop(0, half // step_rows)
        def _(t):
            at = pl.ds(pl.multiple_of(t * step_rows, step_rows), step_rows)
            low = pl.ds(pl.multiple_of(half + t * step_rows, step_rows), step_rows)
            total = part[parity, grp, low, :].astype(f32) + ry[chip, at, :].astype(f32)
            for j in range(1, chips):
                total = total + rv[chip_at(j), at, :].astype(f32)
            finish(low, total)

        if not last:
            ag_start(l + 1)
            relay(l + 1, 0, 1)
        for p in range(2):
            for x in range(chips):
                d_copy(l, p, x).wait_send()
            for j in range(1, chips):
                x_copy(l, p, j).wait_send()
        for j in range(chips):
            w_copy(l, j).wait_send()
        u_copy(l).wait_send()
        for j in range(1, chips):
            v_copy(l, j).wait_send()

    def wait_send(c):
        c.wait_send()

    for l in range(layers):
        for k in range(2):
            y_copy(l, k).wait_send()
            z_each(l, ((k, 0), (k, 1)), wait_send)

            @pl.when(core == 1)
            def _(k=k):
                for side in range(2):
                    h_copy(l, k, side).wait_send()
            for way, (where, _, _) in enumerate(relays):
                @pl.when(line == where)
                def _(way=way):
                    for side in range(2):
                        r_copy(l, k, side, way).wait_send()

        def state_sent(t):
            @pl.when((line + t + 1 < lines) & (core == 1))
            def _():
                line_copy(l, t + 1).wait_send()
                held_copy(l, t + 1).wait_send()

        span(lines - 1, state_sent)

        @pl.when((line + 1 < lines) & (core == 0))
        def _():
            state_copy(l).wait_send()


def local(n_seq, n_grp, hidden, qkv_weight, out_weight, projection, norm_gain, out_gain):
    layers, rows, cols = qkv_weight.shape
    depth, oc = out_weight.shape[1:]
    heads, head, feats = projection.shape[1:]
    tokens, width = hidden.shape
    lines, chips, mine, half = n_seq // 2, n_grp // 2, heads // 2, tokens // 2
    scaled = projection * head ** (-0.25)
    high = lax.reduce_precision(scaled, 8, 7)
    rest = scaled - high
    mid = lax.reduce_precision(rest, 8, 7)
    low = rest - mid
    terms = jnp.concatenate([high, mid, low], axis=-1).astype(bf16)
    gains = out_gain.reshape(layers, heads, 1, head)
    dma = pltpu.SemaphoreType.DMA
    vmem = pl.BlockSpec(memory_space=pltpu.VMEM)
    anywhere = pl.BlockSpec(memory_space=pl.ANY)
    state = (feats + 16, head)
    return pl.pallas_call(
        functools.partial(kernel, n_seq, n_grp),
        out_shape=jax.ShapeDtypeStruct((tokens, width), bf16),
        in_specs=[anywhere, anywhere, anywhere, vmem, vmem, vmem],
        out_specs=vmem,
        scratch_shapes=[
            pltpu.VMEM((layers, n_seq, rows, cols // 2), bf16),
            pltpu.VMEM((layers, n_seq, depth // 2, oc), bf16),
            pltpu.VMEM((layers, 2, rows, cols // 2), bf16),
            pltpu.VMEM((layers, 2, depth // 2, oc), bf16),
            pltpu.VMEM((2, n_grp, tokens, width), bf16),
            pltpu.VMEM((2, n_grp, tokens, width), bf16),
            pltpu.VMEM((2, chips, tokens, width), bf16),
            pltpu.VMEM((2, chips, half, width), bf16),
            pltpu.VMEM((chips, half, width), bf16),
            pltpu.VMEM((chips, half, width), bf16),
            pltpu.VMEM((half, width), bf16),
            pltpu.VMEM((half, width), bf16),
            pltpu.VMEM((chips, half, width), bf16),
            pltpu.VMEM((2 * tokens, n_grp * width), bf16),
            pltpu.VMEM((heads, tokens, feats), bf16),
            pltpu.VMEM((heads, tokens, feats), bf16),
            pltpu.VMEM((heads, tokens, head), bf16),
            pltpu.VMEM((heads, tokens, head), f32),
            pltpu.VMEM((heads, tokens, head), f32),
            pltpu.VMEM((2 * tokens, mine * head), bf16),
            pltpu.VMEM((heads,) + state, f32),
            pltpu.VMEM((layers, mine) + state, bf16),
            pltpu.VMEM((layers, mine) + state, bf16),
            pltpu.VMEM((layers, lines, mine) + state, bf16),
            pltpu.VMEM((mine,) + state, f32),
            dma((1 + 2 * layers,)),
            dma((layers, 2, 2, lines)),
            dma((layers, 2, 2, lines)),
            dma((layers, 2, n_seq)),
            dma((layers, 2, 2, 2)),
            dma((layers, 2)),
            dma((layers, 2)),
            dma((layers, 2, 2)),
            dma((layers, 2, 2)),
            dma((layers, lines)),
            dma((layers, lines)),
            dma((layers, lines)),
            dma((layers,)),
            dma((layers,)),
            dma((2, n_grp, 2, 1 + chips)),
            dma((layers, 2, n_grp, 2)),
            dma((2, chips)),
            dma((layers, 2, chips)),
            dma((2, chips)),
            dma((layers, 2, chips)),
            dma((chips,)),
            dma((layers, chips)),
            dma((1,)),
            dma((layers,)),
            dma((chips,)),
            dma((layers, chips)),
        ],
        compiler_params=pltpu.CompilerParams(
            collective_id=0, has_side_effects=True, vmem_limit_bytes=66_000_000
        ),
    )(hidden, qkv_weight, out_weight, terms, norm_gain, gains)


def solution(mesh):
    return jax.shard_map(
        functools.partial(local, mesh.shape["seq"], mesh.shape["grp"]),
        mesh=mesh,
        in_specs=(
            P("seq", "grp"),
            P(None, "seq", "grp"),
            P(None, "grp", "seq"),
            P(None, "grp", None, None),
            P(),
            P(None, "grp"),
        ),
        out_specs=P("seq", "grp"),
        check_vma=False,
    )
```

```python
import functools
import math

import jax
import jax.numpy as jnp
from jax import lax
from jax.experimental import pallas as pl
from jax.experimental.pallas import tpu as pltpu
from jax.sharding import PartitionSpec as P

MESH = pl.DeviceIdType.MESH
stabilizer = 2.0
f32 = jnp.float32
bf16 = jnp.bfloat16


def remote(src, dst, send, recv, device):
    return pltpu.make_async_remote_copy(
        src_ref=src, dst_ref=dst, send_sem=send, recv_sem=recv, device_id=device, device_id_type=MESH
    )


def kernel(
    n_seq, n_grp, hidden, qkv_w, out_w, proj, norm_gain, out_gain, out,
    wq, wo, xg, part, rsd, rx, ry, rv, ru, ub, vb, normed, qf, kf, vf, num, den, att,
    proj_f, terms, own_state, st_send, st_held, st_in, st_out, st_give, prefix,
    local_sem, z_send, z_recv, r_send, y_send, y_recv, l_send, l_recv, m_send, m_recv, k_send, k_recv,
    ag_send, ag_recv, d_send, d_recv, x_send, x_recv, w_send, w_recv, u_send, u_recv, v_send, v_recv,
):
    layers, rows, cols = qkv_w.shape
    depth, oc = out_w.shape[1:]
    tokens, width = hidden.shape
    heads, head = proj.shape[1:3]
    feats = proj.shape[3]
    lines = n_seq // 2
    chips = n_grp // 2
    mine = heads // 2
    half = tokens // 2
    step_rows = 64
    me = lax.axis_index("seq")
    grp = lax.axis_index("grp")
    line, parity = me // 2, me % 2
    other = 1 - parity
    pair = line * 2 + other
    chip, core = grp // 2, grp % 2
    partner = chip * 2 + 1 - core

    def chip_at(j):
        return lax.rem(chip + j, chips)

    def beside(j):
        return chip_at(j) * 2 + core

    def piece(h):
        return pl.ds(h * half, half)

    def weight(l, k, slot):
        return (wo if k else wq).at[l, slot]

    def own_part(l, k, who):
        if k:
            return out_w.at[l, pl.ds(pl.multiple_of(who * (depth // 2), depth // 2), depth // 2)]
        return qkv_w.at[l, :, pl.ds(pl.multiple_of(who * (cols // 2), cols // 2), cols // 2)]

    own_copies = [
        [pltpu.make_async_copy(own_part(l, k, parity), weight(l, k, me), local_sem.at[1 + 2 * l + k]) for k in range(2)]
        for l in range(layers)
    ]
    own_hidden = pltpu.make_async_copy(hidden, xg.at[parity, grp], local_sem.at[0])
    own_hidden.start()
    own_proj = pltpu.make_async_copy(proj.at[:, pl.ds(parity * mine, mine)], proj_f, local_sem.at[1 + 2 * layers])
    own_proj.start()
    for both in own_copies:
        for c in both:
            c.start()

    barrier = pltpu.get_barrier_semaphore()
    for k in range(1, lines):
        pl.semaphore_signal(barrier, inc=1, device_id={"seq": lax.rem(line + k, lines) * 2 + parity}, device_id_type=MESH)
    pl.semaphore_signal(barrier, inc=1, device_id={"seq": pair}, device_id_type=MESH)
    for k in range(1, n_grp):
        pl.semaphore_signal(barrier, inc=1, device_id={"grp": lax.rem(grp + k, n_grp)}, device_id_type=MESH)
    pl.semaphore_wait(barrier, lines + n_grp - 1)

    def slot_of(where, side):
        return where * 2 + (other if side else parity)

    def y_copy(l, k):
        return remote(own_part(l, k, other), weight(l, k, me), y_send.at[l, k], y_recv.at[l, k], {"seq": pair})

    def y_arrival(l, k):
        return remote(weight(l, k, pair), weight(l, k, pair), y_send.at[l, k], y_recv.at[l, k], {"seq": pair})

    def z_copy(l, k, side, way):
        ref = weight(l, k, slot_of(line, side))
        to = line - 1 if way else line + 1
        return remote(ref, ref, z_send.at[l, k, side, way], z_recv.at[l, k, slot_of(line, side)], {"seq": to * 2 + parity})

    def z_arrival(l, k, side, src):
        ref = weight(l, k, slot_of(src, side))
        return remote(ref, ref, z_send.at[l, k, side, 0], z_recv.at[l, k, slot_of(src, side)], {"seq": pair})

    def r_copy(l, k, side, hop, way):
        src, to = (line + hop, line - 1) if way else (line - hop, line + 1)
        ref = weight(l, k, slot_of(src, side))
        return remote(
            ref, ref, r_send.at[l, k, side, way, hop], z_recv.at[l, k, slot_of(src, side)], {"seq": to * 2 + parity}
        )

    def span(count, body):
        if count <= 4:
            for t in range(count):
                body(t)
        else:
            pl.loop(0, count)(body)

    def z_up(act, l, *pieces):
        @pl.when(line + 1 < lines)
        def _():
            for k, side in pieces:
                act(z_copy(l, k, side, 0))

    def z_down(act, l, *pieces):
        @pl.when(line >= 1)
        def _():
            for k, side in pieces:
                act(z_copy(l, k, side, 1))

    def start(c):
        c.start()

    def z_start(l, *pieces):
        z_up(start, l, *pieces)
        z_down(start, l, *pieces)

    upper = 2 * line >= lines

    def r_each(hop, act, where=None):
        up, down = (line >= hop) & (line + 1 < lines), (line + hop < lines) & (line >= 1)
        if where is not None:
            up, down = up & (upper == where), down & (upper != where)

        @pl.when(up)
        def _():
            act(line - hop, 0)

        @pl.when(down)
        def _():
            act(line + hop, 1)

    def forward(l, k, hop, where=None):
        for side in range(2):
            def act(src, way, side=side):
                z_arrival(l, k, side, src).wait_recv()
                r_copy(l, k, side, hop, way).start()

            r_each(hop, act, where)

    def outward(l, *kinds):
        for k in kinds:
            forward(l, k, 1, True)

    def inward(l, *kinds):
        for k in kinds:
            forward(l, k, 1, False)

    def far(l, *kinds):
        for k in kinds:
            span(lines - 3, lambda t: forward(l, k, t + 2))

    def weights_wait(l, k):
        def body(src):
            @pl.when((src != line) & ((line == 0) | (line == lines - 1)))
            def _():
                for side in range(2):
                    z_arrival(l, k, side, src).wait_recv()

        span(lines, body)

    def prepare(l):
        for c in own_copies[l]:
            c.wait()
        for k in range(2):
            y_arrival(l, k).wait_recv()

    def ag_copy(l, p, g, h, kind, device):
        ref = xg.at[p, g, piece(h)]
        return remote(ref, ref, ag_send.at[p, g, h, kind], ag_recv.at[l, p, g, h], device)

    to_pair, to_partner = {"seq": pair}, {"grp": partner}

    def ag_wait(l, p, g, h):
        ag_copy(l, p, g, h, 0, to_pair).wait_recv()

    def ag_sends(l):
        first, second = [], []
        for j in range(1, chips):
            first.append((parity, grp, 1, 1 + j, {"grp": beside(j)}))
        first.append((parity, grp, 0, 1, to_pair))
        for j in range(1, chips):
            first.append((parity, grp, 0, 1 + j, {"grp": beside(j)}))
        first.append((parity, grp, 1, 1, to_pair))
        for h in range(2):
            first.append((parity, grp, h, 0, to_partner))
        forward = [((other, grp, 0), [(1 + j, {"grp": beside(j)}) for j in range(1, chips)])]
        for j in range(1, chips):
            forward.append(((parity, beside(j), 1), [(1, to_pair)]))
        forward.append(((other, grp, 1), []))
        for j in range(1, chips):
            forward.append(((parity, beside(j), 0), []))
        for j in range(1, chips):
            for h in range(2):
                forward.append(((other, beside(j), h), []))
        for slot, targets in forward:
            second.append((slot, [slot + t for t in targets + [(0, to_partner)]]))
        return first, second

    def ag_start(l):
        for args in ag_sends(l)[0]:
            ag_copy(l, *args).start()

    def ag_finish(l):
        first, second = ag_sends(l)
        for slot, targets in second:
            ag_wait(l, *slot)
            for args in targets:
                ag_copy(l, *args).start()
        for h in range(2):
            for p in (parity, other):
                ag_wait(l, p, partner, h)
                for j in range(1, chips):
                    ag_wait(l, p, chip_at(j) * 2 + 1 - core, h)

    def ag_drain(l):
        first, second = ag_sends(l)
        for args in first + [a for _, targets in second for a in targets]:
            ag_copy(l, *args).wait_send()

    def d_copy(l, p, x):
        return remote(part.at[p, x * 2 + 1 - core], rsd.at[p, x], d_send.at[p, x], d_recv.at[l, p, x], to_partner)

    def x_copy(l, p, j):
        return remote(
            part.at[p, beside(j), piece(0)], rx.at[p, chip], x_send.at[p, j], x_recv.at[l, p, chip], {"grp": beside(j)}
        )

    def x_arrival(l, p, j):
        ref = rx.at[p, chip_at(j)]
        return remote(ref, ref, x_send.at[p, j], x_recv.at[l, p, chip_at(j)], {"grp": beside(j)})

    def w_copy(l, j):
        x = chip_at(j)
        return remote(part.at[other, beside(j), piece(1)], ry.at[x], w_send.at[x], w_recv.at[l, x], to_pair)

    def u_copy(l):
        return remote(ub, ru, u_send.at[0], u_recv.at[l], to_pair)

    def v_copy(l, j):
        return remote(vb.at[chip_at(j)], rv.at[chip], v_send.at[j], v_recv.at[l, chip], {"grp": beside(j)})

    def v_arrival(l, j):
        ref = rv.at[chip_at(j)]
        return remote(ref, ref, v_send.at[j], v_recv.at[l, chip_at(j)], {"grp": beside(j)})

    def state_copy(l):
        return remote(st_send.at[l], st_held.at[l], k_send.at[l], k_recv.at[l], to_partner)

    def chain_copy(l):
        return remote(st_out.at[l], st_in.at[l], l_send.at[l], l_recv.at[l], {"seq": line * 2 + 2 + parity})

    def give_copy(l):
        return remote(st_in.at[l, 0], st_give.at[l], m_send.at[l], m_recv.at[l], to_partner)

    below, above = line >= 1, line + 1 < lines

    def wait_send(c):
        c.wait_send()

    def drain(l):
        for k in range(2):
            y_copy(l, k).wait_send()
            z_up(wait_send, l, (k, 0), (k, 1))
            z_down(wait_send, l, (k, 0), (k, 1))
            for side in range(2):
                def forwarded(t, k=k, side=side):
                    r_each(t + 1, lambda src, way: r_copy(l, k, side, t + 1, way).wait_send())

                span(lines - 2, forwarded)

        @pl.when(above & (core == 0))
        def _():
            state_copy(l).wait_send()

        @pl.when(above & (core == 1))
        def _():
            chain_copy(l).wait_send()

        @pl.when(below & (core == 1))
        def _():
            give_copy(l).wait_send()

    for k in range(2):
        y_copy(0, k).start()
    for c in own_copies[0]:
        c.wait()
    z_start(0, (0, 0))
    own_hidden.wait()
    ag_start(0)
    if layers > 1:
        for k in range(2):
            y_copy(1, k).start()
    y_arrival(0, 0).wait_recv()
    z_start(0, (0, 1))
    y_arrival(0, 1).wait_recv()
    z_start(0, (1, 0), (1, 1))
    for k in range(2):
        outward(0, k)
        inward(0, k)

    scale = head ** (-0.25)
    inv = 1.0 / math.sqrt(feats)

    def features(u, terms):
        mixed = jnp.dot(u, terms, preferred_element_type=f32)
        mixed = (mixed[:, 2 * feats :] + mixed[:, feats : 2 * feats]) + mixed[:, :feats]
        w0 = u.astype(f32) * scale
        energy = 0.5 * jnp.sum(w0 * w0, axis=-1, keepdims=True)
        return (jnp.exp(mixed - energy - stabilizer) * inv).astype(bf16)

    for l in range(layers):
        last = l == layers - 1
        ag_finish(l)
        if l == 0:
            for n in range(2, layers):
                for k in range(2):
                    y_copy(n, k).start()
        elif last:
            outward(l, 1)
            inward(l, 1)

        @pl.loop(0, 2 * tokens // step_rows)
        def _(t):
            at = pl.ds(pl.multiple_of(t * step_rows, step_rows), step_rows)
            b = t // (tokens // step_rows)
            src = pl.ds(pl.multiple_of(t % (tokens // step_rows) * step_rows, step_rows), step_rows)
            wide = [xg[b, g, src, :].astype(f32) for g in range(n_grp)]
            total = sum(jnp.sum(v * v, axis=-1, keepdims=True) for v in wide)
            rms = lax.rsqrt(total / (width * n_grp) + 1e-05)
            for g in range(n_grp):
                cut = slice(g * width, (g + 1) * width)
                normed[at, cut] = (wide[g] * rms * norm_gain[l : l + 1, cut]).astype(bf16)

        ag_drain(l)
        if l == 0:
            far(0, 0, 1)
        split = l + 1 == layers - 1
        early = ((0, 0), (0, 1)) if split else ((0, 0), (0, 1), (1, 0), (1, 1))
        if not last:
            prepare(l + 1)
            z_down(start, l + 1, *early)

            @pl.when(core == 0)
            def _():
                z_up(start, l + 1, *early)

        if l == 0:
            own_proj.wait()

            @pl.loop(0, layers * mine)
            def _(i):
                n, h = i // mine, i % mine
                scaled = proj_f[n, h] * scale
                high = scaled.astype(bf16)
                rest = scaled - high.astype(f32)
                mid = rest.astype(bf16)
                terms[n, h, :, :feats] = high
                terms[n, h, :, feats : 2 * feats] = mid
                terms[n, h, :, 2 * feats :] = (rest - mid.astype(f32)).astype(bf16)

        weights_wait(l, 0)

        @pl.loop(0, 2 * mine)
        def _(i):
            h, b = i // 2, i % 2
            at = pl.ds(pl.multiple_of(h * 3 * head, 128), 3 * head)
            w = wq[l, :, :, at].reshape(n_seq * rows, 3 * head)
            x = normed[pl.ds(pl.multiple_of(b * tokens, tokens), tokens), :]
            qkv = jnp.dot(x, w, preferred_element_type=f32).astype(bf16)
            split_terms = terms[l, h]
            key = features(qkv[:, head : 2 * head], split_terms)
            value = qkv[:, 2 * head :]
            qf[i] = features(qkv[:, :head], split_terms)
            kf[i] = key
            vf[i] = value
            own_state[i, :feats] = lax.dot_general(key, value, (((0,), (0,)), ((), ())), preferred_element_type=f32)
            own_state[i, feats:] = jnp.dot(jnp.ones((16, tokens), bf16), key, preferred_element_type=f32)

        for h in range(mine):
            st_send[l, h] = (own_state[2 * h] + own_state[2 * h + 1]).astype(bf16)

        @pl.when(above & (core == 0))
        def _():
            state_copy(l).start()

        @pl.when(above & (core == 1) & (line == 0))
        def _():
            state_copy(l).wait_recv()
            st_out[l, 0] = st_held[l]
            st_out[l, 1] = st_send[l]
            chain_copy(l).start()

        @pl.loop(0, 2 * mine)
        def _(i):
            scores = lax.dot_general(qf[i], kf[i], (((1,), (1,)), ((), ())), preferred_element_type=f32)
            r = lax.broadcasted_iota(jnp.int32, (tokens, tokens), 0)
            c = lax.broadcasted_iota(jnp.int32, (tokens, tokens), 1)
            masked = jnp.where(r >= c, scores, 0.0)
            den[i] = jnp.broadcast_to(jnp.sum(masked, axis=-1, keepdims=True), (tokens, head))
            num[i] = jnp.dot(masked.astype(bf16), vf[i], preferred_element_type=f32)

        kinds = (0,) if split else (0, 1)
        if last:
            far(l, 1)

        @pl.when(line == 0)
        def _():
            for h in range(mine):
                prefix[h] = jnp.zeros_like(prefix[h])

        @pl.when(below & (core == 1))
        def _():
            chain_copy(l).wait_recv()
            give_copy(l).start()
            for h in range(mine):
                prefix[h] = st_in[l, 1, h].astype(f32)

        @pl.when(below & above & (core == 1))
        def _():
            state_copy(l).wait_recv()
            for h in range(mine):
                st_out[l, 0, h] = (st_in[l, 0, h].astype(f32) + st_held[l, h].astype(f32)).astype(bf16)
                st_out[l, 1, h] = (prefix[h] + own_state[2 * h] + own_state[2 * h + 1]).astype(bf16)
            chain_copy(l).start()

        if not last:
            @pl.when(core == 1)
            def _():
                z_up(start, l + 1, *early)

        @pl.when(below & (core == 0))
        def _():
            give_copy(l).wait_recv()
            for h in range(mine):
                prefix[h] = st_give[l, h].astype(f32)

        @pl.loop(0, 2 * mine)
        def _(i):
            h, b = i // 2, i % 2
            before = prefix[h] + own_state[2 * h] * jnp.where(b == 1, 1.0, 0.0)
            q = qf[i]
            d = den[i] + jnp.sum(q.astype(f32) * before[feats : feats + 1], axis=-1, keepdims=True)
            n = num[i] + jnp.dot(q, before[:feats].astype(bf16), preferred_element_type=f32)
            a = n / d
            norm = lax.rsqrt(jnp.mean(a * a, axis=-1, keepdims=True) + 1e-06)
            to_rows = pl.ds(pl.multiple_of(b * tokens, tokens), tokens)
            to_cols = pl.ds(pl.multiple_of(h * head, 128), head)
            to_gain = pl.ds(pl.multiple_of((parity * mine + h) * head, 128), head)
            att[to_rows, to_cols] = (a * norm * out_gain[l : l + 1, to_gain]).astype(bf16)

        weights_wait(l, 1)
        per = width // oc

        def project(p, g):
            a = att[pl.ds(pl.multiple_of(p * tokens, tokens), tokens), :]
            for i in range(per):
                part[p, g, :, i * oc : (i + 1) * oc] = jnp.dot(
                    a, wo[l, g * per + i], preferred_element_type=f32
                ).astype(bf16)

        @pl.loop(0, 2 * chips)
        def _(n):
            p = lax.rem(other + n // chips, 2)
            x = lax.rem(chip + 1 + n % chips, chips)
            project(p, x * 2 + 1 - core)
            d_copy(l, p, x).start()

        @pl.loop(0, 2 * chips)
        def _(n):
            p = lax.rem(other + n // chips, 2)
            x = lax.rem(chip + 1 + n % chips, chips)
            project(p, x * 2 + core)

        if not last:
            inward(l + 1, *kinds)
        hops = list(range(1, chips)) + [0]
        for own in range(2):
            p = parity if own else other
            for j in hops:
                x = chip_at(j)
                d_copy(l, p, x).wait_recv()

                @pl.loop(0, tokens // step_rows)
                def _(t, p=p, x=x, j=j):
                    at = pl.ds(pl.multiple_of(t * step_rows, step_rows), step_rows)
                    part[p, beside(j), at, :] = (
                        part[p, beside(j), at, :].astype(f32) + rsd[p, x, at, :].astype(f32)
                    ).astype(bf16)

                if j:
                    x_copy(l, p, j).start()
                if not own:
                    w_copy(l, j).start()

        if last:
            for n in range(l):
                drain(n)
        else:
            outward(l + 1, *kinds)
        for j in range(1, chips):
            x_arrival(l, other, j).wait_recv()

        @pl.loop(0, half // step_rows)
        def _(t):
            at = pl.ds(pl.multiple_of(t * step_rows, step_rows), step_rows)
            total = part[other, grp, at, :].astype(f32)
            for j in range(1, chips):
                total = total + rx[other, chip_at(j), at, :].astype(f32)
            ub[at, :] = total.astype(bf16)

        u_copy(l).start()
        for j in hops:
            w_arrival = remote(ry.at[chip_at(j)], ry.at[chip_at(j)], w_send.at[j], w_recv.at[l, chip_at(j)], to_pair)
            w_arrival.wait_recv()
            if j:
                @pl.loop(0, half // step_rows)
                def _(t, j=j):
                    at = pl.ds(pl.multiple_of(t * step_rows, step_rows), step_rows)
                    low = pl.ds(pl.multiple_of(half + t * step_rows, step_rows), step_rows)
                    vb[chip_at(j), at, :] = (
                        part[parity, beside(j), low, :].astype(f32) + ry[chip_at(j), at, :].astype(f32)
                    ).astype(bf16)

                v_copy(l, j).start()
        if last:
            drain(l)
        for j in range(1, chips):
            x_arrival(l, parity, j).wait_recv()
        u_copy(l).wait_recv()

        def finish(at, total):
            total = (xg[parity, grp, at, :].astype(f32) + total).astype(bf16)
            if last:
                out[at, :] = total
            else:
                xg[parity, grp, at, :] = total

        @pl.loop(0, half // step_rows)
        def _(t):
            at = pl.ds(pl.multiple_of(t * step_rows, step_rows), step_rows)
            total = part[parity, grp, at, :].astype(f32) + ru[at, :].astype(f32)
            for j in range(1, chips):
                total = total + rx[parity, chip_at(j), at, :].astype(f32)
            finish(at, total)

        for j in range(1, chips):
            v_arrival(l, j).wait_recv()

        @pl.loop(0, half // step_rows)
        def _(t):
            at = pl.ds(pl.multiple_of(t * step_rows, step_rows), step_rows)
            low = pl.ds(pl.multiple_of(half + t * step_rows, step_rows), step_rows)
            total = part[parity, grp, low, :].astype(f32) + ry[chip, at, :].astype(f32)
            for j in range(1, chips):
                total = total + rv[chip_at(j), at, :].astype(f32)
            finish(low, total)

        if not last:
            ag_start(l + 1)
            far(l + 1, *kinds)
            if split:
                z_start(l + 1, (1, 0), (1, 1))
        for p in range(2):
            for x in range(chips):
                d_copy(l, p, x).wait_send()
            for j in range(1, chips):
                x_copy(l, p, j).wait_send()
        for j in range(chips):
            w_copy(l, j).wait_send()
        u_copy(l).wait_send()
        for j in range(1, chips):
            v_copy(l, j).wait_send()

def local(n_seq, n_grp, hidden, qkv_weight, out_weight, projection, norm_gain, out_gain):
    layers, rows, cols = qkv_weight.shape
    depth, oc = out_weight.shape[1:]
    heads, head, feats = projection.shape[1:]
    tokens, width = hidden.shape
    lines, chips, mine, half = n_seq // 2, n_grp // 2, heads // 2, tokens // 2
    dma = pltpu.SemaphoreType.DMA
    vmem = pl.BlockSpec(memory_space=pltpu.VMEM)
    anywhere = pl.BlockSpec(memory_space=pl.ANY)
    state = (feats + 16, head)
    return pl.pallas_call(
        functools.partial(kernel, n_seq, n_grp),
        out_shape=jax.ShapeDtypeStruct((tokens, width), bf16),
        in_specs=[anywhere, anywhere, anywhere, anywhere, vmem, vmem],
        out_specs=vmem,
        scratch_shapes=[
            pltpu.VMEM((layers, n_seq, rows, cols // 2), bf16),
            pltpu.VMEM((layers, n_seq, depth // 2, oc), bf16),
            pltpu.VMEM((2, n_grp, tokens, width), bf16),
            pltpu.VMEM((2, n_grp, tokens, width), bf16),
            pltpu.VMEM((2, chips, tokens, width), bf16),
            pltpu.VMEM((2, chips, half, width), bf16),
            pltpu.VMEM((chips, half, width), bf16),
            pltpu.VMEM((chips, half, width), bf16),
            pltpu.VMEM((half, width), bf16),
            pltpu.VMEM((half, width), bf16),
            pltpu.VMEM((chips, half, width), bf16),
            pltpu.VMEM((2 * tokens, n_grp * width), bf16),
            pltpu.VMEM((heads, tokens, feats), bf16),
            pltpu.VMEM((heads, tokens, feats), bf16),
            pltpu.VMEM((heads, tokens, head), bf16),
            pltpu.VMEM((heads, tokens, head), f32),
            pltpu.VMEM((heads, tokens, head), f32),
            pltpu.VMEM((2 * tokens, mine * head), bf16),
            pltpu.VMEM((layers, mine, head, feats), f32),
            pltpu.VMEM((layers, mine, head, 3 * feats), bf16),
            pltpu.VMEM((heads,) + state, f32),
            pltpu.VMEM((layers, mine) + state, bf16),
            pltpu.VMEM((layers, mine) + state, bf16),
            pltpu.VMEM((layers, 2, mine) + state, bf16),
            pltpu.VMEM((layers, 2, mine) + state, bf16),
            pltpu.VMEM((layers, mine) + state, bf16),
            pltpu.VMEM((mine,) + state, f32),
            dma((2 + 2 * layers,)),
            dma((layers, 2, 2, 2)),
            dma((layers, 2, n_seq)),
            dma((layers, 2, 2, 2, lines)),
            dma((layers, 2)),
            dma((layers, 2)),
            dma((layers,)),
            dma((layers,)),
            dma((layers,)),
            dma((layers,)),
            dma((layers,)),
            dma((layers,)),
            dma((2, n_grp, 2, 1 + chips)),
            dma((layers, 2, n_grp, 2)),
            dma((2, chips)),
            dma((layers, 2, chips)),
            dma((2, chips)),
            dma((layers, 2, chips)),
            dma((chips,)),
            dma((layers, chips)),
            dma((1,)),
            dma((layers,)),
            dma((chips,)),
            dma((layers, chips)),
        ],
        compiler_params=pltpu.CompilerParams(
            collective_id=0, has_side_effects=True, vmem_limit_bytes=66_000_000
        ),
    )(hidden, qkv_weight, out_weight, projection, norm_gain, out_gain)


def solution(mesh):
    return jax.shard_map(
        functools.partial(local, mesh.shape["seq"], mesh.shape["grp"]),
        mesh=mesh,
        in_specs=(
            P("seq", "grp"),
            P(None, "seq", "grp"),
            P(None, "grp", "seq"),
            P(None, "grp", None, None),
            P(),
            P(None, "grp"),
        ),
        out_specs=P("seq", "grp"),
        check_vma=False,
    )
```

```python
import functools
import math

import jax
import jax.numpy as jnp
from jax import lax
from jax.experimental import pallas as pl
from jax.experimental.pallas import tpu as pltpu
from jax.sharding import PartitionSpec as P

MESH = pl.DeviceIdType.MESH
stabilizer = 2.0
f32 = jnp.float32
bf16 = jnp.bfloat16


def remote(src, dst, send, recv, device):
    return pltpu.make_async_remote_copy(
        src_ref=src, dst_ref=dst, send_sem=send, recv_sem=recv, device_id=device, device_id_type=MESH
    )


def kernel(
    n_seq, n_grp, hidden, qkv_w, out_w, proj, norm_gain, out_gain, out,
    wq, wo, xg, part, rsd, rx, ry, rv, ru, ub, vb, normed, qf, kf, vf, num, den, att,
    proj_f, terms, own_state, st_send, st_held, st_in, st_out, st_give, prefix,
    local_sem, z_send, z_recv, r_send, y_send, y_recv, l_send, l_recv, m_send, m_recv, k_send, k_recv,
    ag_send, ag_recv, d_send, d_recv, x_send, x_recv, w_send, w_recv, u_send, u_recv, v_send, v_recv,
):
    layers, rows, cols = qkv_w.shape
    depth, oc = out_w.shape[1:]
    tokens, width = hidden.shape
    heads, head = proj.shape[1:3]
    feats = proj.shape[3]
    lines = n_seq // 2
    chips = n_grp // 2
    mine = heads // 2
    half = tokens // 2
    step_rows = 64
    me = lax.axis_index("seq")
    grp = lax.axis_index("grp")
    line, parity = me // 2, me % 2
    other = 1 - parity
    pair = line * 2 + other
    chip, core = grp // 2, grp % 2
    partner = chip * 2 + 1 - core

    def chip_at(j):
        return lax.rem(chip + j, chips)

    def beside(j):
        return chip_at(j) * 2 + core

    def piece(h):
        return pl.ds(h * half, half)

    def weight(l, k, slot):
        return (wo if k else wq).at[l, slot]

    def line_pair(l, k, where):
        return (wo if k else wq).at[l, pl.ds(where * 2, 2)]

    def own_part(l, k, who):
        if k:
            return out_w.at[l, pl.ds(pl.multiple_of(who * (depth // 2), depth // 2), depth // 2)]
        return qkv_w.at[l, :, pl.ds(pl.multiple_of(who * (cols // 2), cols // 2), cols // 2)]

    own_copies = [
        [pltpu.make_async_copy(own_part(l, k, parity), weight(l, k, me), local_sem.at[1 + 2 * l + k]) for k in range(2)]
        for l in range(layers)
    ]
    own_hidden = pltpu.make_async_copy(hidden, xg.at[parity, grp], local_sem.at[0])
    own_hidden.start()
    own_proj = pltpu.make_async_copy(proj.at[:, pl.ds(parity * mine, mine)], proj_f, local_sem.at[1 + 2 * layers])
    own_proj.start()
    for pieces in own_copies:
        for c in pieces:
            c.start()

    barrier = pltpu.get_barrier_semaphore()
    for k in range(1, lines):
        pl.semaphore_signal(barrier, inc=1, device_id={"seq": lax.rem(line + k, lines) * 2 + parity}, device_id_type=MESH)
    pl.semaphore_signal(barrier, inc=1, device_id={"seq": pair}, device_id_type=MESH)
    for k in range(1, n_grp):
        pl.semaphore_signal(barrier, inc=1, device_id={"grp": lax.rem(grp + k, n_grp)}, device_id_type=MESH)
    pl.semaphore_wait(barrier, lines + n_grp - 1)

    def slot_of(where, side):
        return where * 2 + (other if side else parity)

    def y_copy(l, k):
        return remote(own_part(l, k, other), weight(l, k, me), y_send.at[l, k], y_recv.at[l, k], {"seq": pair})

    def y_arrival(l, k):
        return remote(weight(l, k, pair), weight(l, k, pair), y_send.at[l, k], y_recv.at[l, k], {"seq": pair})

    def z_copy(l, k, way, side=None):
        ref = line_pair(l, k, line) if side is None else weight(l, k, slot_of(line, side))
        to = line - 1 if way else line + 1
        return remote(ref, ref, z_send.at[l, k, way], z_recv.at[l, k, line], {"seq": to * 2 + parity})

    def z_arrival(l, k, src):
        ref = line_pair(l, k, src)
        return remote(ref, ref, z_send.at[l, k, 0], z_recv.at[l, k, src], {"seq": pair})

    def r_copy(l, k, src, way):
        ref = line_pair(l, k, src)
        to = line - 1 if way else line + 1
        return remote(ref, ref, r_send.at[l, k, src], z_recv.at[l, k, src], {"seq": to * 2 + parity})

    def span(count, body):
        if count <= 4:
            for t in range(count):
                body(t)
        else:
            pl.loop(0, count)(body)

    def z_up(act, l, *kinds, side=None):
        @pl.when(line + 1 < lines)
        def _():
            for k in kinds:
                act(z_copy(l, k, 0, side))

    def z_down(act, l, *kinds, side=None):
        @pl.when(line >= 1)
        def _():
            for k in kinds:
                act(z_copy(l, k, 1, side))

    def start(c):
        c.start()

    def z_start(l, *kinds, side=None):
        z_up(start, l, *kinds, side=side)
        z_down(start, l, *kinds, side=side)

    upper = 2 * line >= lines

    def r_each(hop, act, where=None):
        up, down = (line >= hop) & (line + 1 < lines), (line + hop < lines) & (line >= 1)
        if where is not None:
            up, down = up & (upper == where), down & (upper != where)

        @pl.when(up)
        def _():
            act(line - hop, 0)

        @pl.when(down)
        def _():
            act(line + hop, 1)

    def forward(l, k, hop, where=None):
        def act(src, way):
            z_arrival(l, k, src).wait_recv()
            r_copy(l, k, src, way).start()

        r_each(hop, act, where)

    def outward(l, *kinds):
        for k in kinds:
            forward(l, k, 1, True)

    def inward(l, *kinds):
        for k in kinds:
            forward(l, k, 1, False)

    def far(l, *kinds):
        for k in kinds:
            span(lines - 3, lambda t: forward(l, k, t + 2))

    def weights_wait(l, k):
        def body(src):
            @pl.when((src != line) & ((line == 0) | (line == lines - 1)))
            def _():
                z_arrival(l, k, src).wait_recv()

        span(lines, body)

    def prepare(l):
        for c in own_copies[l]:
            c.wait()
        for k in range(2):
            y_arrival(l, k).wait_recv()

    def ag_copy(l, p, g, h, place, device):
        ref = xg.at[p, g, piece(h)]
        return remote(ref, ref, ag_send.at[place], ag_recv.at[p, g, h], device)

    to_pair, to_partner = {"seq": pair}, {"grp": partner}

    def ag_wait(l, p, g, h):
        ag_copy(l, p, g, h, 0, to_pair).wait_recv()

    def ag_sends(l):
        across = [{"grp": beside(j)} for j in range(1, chips)]
        own = [(1, d) for d in across] + [(0, to_pair)] + [(0, d) for d in across] + [(1, to_pair)]
        own += [(h, to_partner) for h in range(2)]
        passed = [((other, grp, 0), across)]
        passed += [((parity, beside(j), 1), [to_pair]) for j in range(1, chips)]
        passed += [((other, grp, 1), [])] + [((parity, beside(j), 0), []) for j in range(1, chips)]
        passed += [((other, beside(j), h), []) for j in range(1, chips) for h in range(2)]
        first = [(parity, grp, h, n, d) for n, (h, d) in enumerate(own)]
        second, n = [], len(first)
        for slot, targets in passed:
            second.append((slot, [slot + (n + i, d) for i, d in enumerate(targets + [to_partner])]))
            n += len(targets) + 1
        return first, second

    def ag_start(l):
        for args in ag_sends(l)[0]:
            ag_copy(l, *args).start()

    def ag_own(l):
        for slot, targets in ag_sends(l)[1][: 2 * chips]:
            ag_pass(l, slot, targets)
        ag_beside(l, parity)

    def ag_other(l):
        for slot, targets in ag_sends(l)[1][2 * chips :]:
            ag_pass(l, slot, targets)
        ag_beside(l, other)

    def ag_pass(l, slot, targets):
        ag_wait(l, *slot)
        for args in targets:
            ag_copy(l, *args).start()

    def ag_beside(l, p):
        for h in range(2):
            ag_wait(l, p, partner, h)
            for j in range(1, chips):
                ag_wait(l, p, chip_at(j) * 2 + 1 - core, h)

    def ag_drain(l):
        first, second = ag_sends(l)
        for args in first + [a for _, targets in second for a in targets]:
            ag_copy(l, *args).wait_send()

    def d_copy(l, p, x):
        return remote(part.at[p, x * 2 + 1 - core], rsd.at[p, x], d_send.at[p, x], d_recv.at[p, x], to_partner)

    def x_copy(l, p, j):
        return remote(
            part.at[p, beside(j), piece(0)], rx.at[p, chip], x_send.at[p, j], x_recv.at[p, chip], {"grp": beside(j)}
        )

    def x_arrival(l, p, j):
        ref = rx.at[p, chip_at(j)]
        return remote(ref, ref, x_send.at[p, j], x_recv.at[p, chip_at(j)], {"grp": beside(j)})

    def w_copy(l, j):
        x = chip_at(j)
        return remote(part.at[other, beside(j), piece(1)], ry.at[x], w_send.at[x], w_recv.at[x], to_pair)

    def u_copy(l):
        return remote(ub, ru, u_send.at[0], u_recv.at[0], to_pair)

    def v_copy(l, j):
        return remote(vb.at[chip_at(j)], rv.at[chip], v_send.at[j], v_recv.at[chip], {"grp": beside(j)})

    def v_arrival(l, j):
        ref = rv.at[chip_at(j)]
        return remote(ref, ref, v_send.at[j], v_recv.at[chip_at(j)], {"grp": beside(j)})

    def state_copy(l):
        return remote(st_send.at[l], st_held.at[l], k_send.at[l], k_recv.at[l], to_partner)

    def chain_copy(l):
        return remote(st_out.at[l], st_in.at[l], l_send.at[l], l_recv.at[l], {"seq": line * 2 + 2 + parity})

    def give_copy(l):
        return remote(st_in.at[l, 0], st_give.at[l], m_send.at[l], m_recv.at[l], to_partner)

    below, above = line >= 1, line + 1 < lines
    held_back = (core == 1) & (line == lines - 2)

    def wait_send(c):
        c.wait_send()

    def drain(l):
        for k in range(2):
            y_copy(l, k).wait_send()
            z_up(wait_send, l, k)
            z_down(wait_send, l, k)

            def forwarded(t, k=k):
                r_each(t + 1, lambda src, way: r_copy(l, k, src, way).wait_send())

            span(lines - 2, forwarded)

        @pl.when(above & (core == 0))
        def _():
            state_copy(l).wait_send()

        @pl.when(above & (core == 1))
        def _():
            chain_copy(l).wait_send()

        @pl.when(below & (core == 1))
        def _():
            give_copy(l).wait_send()

    for k in range(2):
        y_copy(0, k).start()
    for c in own_copies[0]:
        c.wait()
    z_start(0, 0, side=0)
    own_hidden.wait()
    ag_start(0)
    if layers > 1:
        for k in range(2):
            y_copy(1, k).start()
    y_arrival(0, 0).wait_recv()
    z_start(0, 0, side=1)
    y_arrival(0, 1).wait_recv()
    z_start(0, 1)
    for k in range(2):
        outward(0, k)
        inward(0, k)

    scale = head ** (-0.25)
    inv = 1.0 / math.sqrt(feats)

    def features(u, terms):
        mixed = jnp.dot(u, terms, preferred_element_type=f32)
        mixed = (mixed[:, 2 * feats :] + mixed[:, feats : 2 * feats]) + mixed[:, :feats]
        w0 = u.astype(f32) * scale
        energy = 0.5 * jnp.sum(w0 * w0, axis=-1, keepdims=True)
        return (jnp.exp(mixed - energy - stabilizer) * inv).astype(bf16)

    for l in range(layers):
        last = l == layers - 1
        def normalize(b):
            @pl.loop(0, tokens // step_rows)
            def _(t):
                at = pl.ds(pl.multiple_of(b * tokens + t * step_rows, step_rows), step_rows)
                src = pl.ds(pl.multiple_of(t * step_rows, step_rows), step_rows)
                wide = [xg[b, g, src, :].astype(f32) for g in range(n_grp)]
                total = sum(jnp.sum(v * v, axis=-1, keepdims=True) for v in wide)
                rms = lax.rsqrt(total / (width * n_grp) + 1e-05)
                for g in range(n_grp):
                    cut = slice(g * width, (g + 1) * width)
                    normed[at, cut] = (wide[g] * rms * norm_gain[l : l + 1, cut]).astype(bf16)

        ag_own(l)
        normalize(parity)
        ag_other(l)
        if l == 0:
            for n in range(2, layers):
                for k in range(2):
                    y_copy(n, k).start()
        elif last:
            outward(l, 1)
            inward(l, 1)
        normalize(other)
        ag_drain(l)
        if l == 0:
            far(0, 0, 1)
        split = l + 1 == layers - 1
        early = (0,) if split else (0, 1)
        if not last:
            prepare(l + 1)
            z_down(start, l + 1, *early)

            @pl.when(jnp.logical_not(held_back))
            def _():
                z_up(start, l + 1, *early)

        if l == 0:
            own_proj.wait()

            @pl.loop(0, layers * mine)
            def _(i):
                n, h = i // mine, i % mine
                scaled = proj_f[n, h] * scale
                high = scaled.astype(bf16)
                rest = scaled - high.astype(f32)
                mid = rest.astype(bf16)
                terms[n, h, :, :feats] = high
                terms[n, h, :, feats : 2 * feats] = mid
                terms[n, h, :, 2 * feats :] = (rest - mid.astype(f32)).astype(bf16)

        weights_wait(l, 0)

        @pl.loop(0, 2 * mine)
        def _(i):
            h, b = i // 2, i % 2
            at = pl.ds(pl.multiple_of(h * 3 * head, 128), 3 * head)
            w = wq[l, :, :, at].reshape(n_seq * rows, 3 * head)
            x = normed[pl.ds(pl.multiple_of(b * tokens, tokens), tokens), :]
            qkv = jnp.dot(x, w, preferred_element_type=f32).astype(bf16)
            split_terms = terms[l, h]
            key = features(qkv[:, head : 2 * head], split_terms)
            value = qkv[:, 2 * head :]
            qf[i] = features(qkv[:, :head], split_terms)
            kf[i] = key
            vf[i] = value
            own_state[i, :feats] = lax.dot_general(key, value, (((0,), (0,)), ((), ())), preferred_element_type=f32)
            own_state[i, feats:] = jnp.dot(jnp.ones((16, tokens), bf16), key, preferred_element_type=f32)

        for h in range(mine):
            st_send[l, h] = (own_state[2 * h] + own_state[2 * h + 1]).astype(bf16)

        @pl.when(above & (core == 0))
        def _():
            state_copy(l).start()

        @pl.when(above & (core == 1) & (line == 0))
        def _():
            state_copy(l).wait_recv()
            st_out[l, 0] = st_held[l]
            st_out[l, 1] = st_send[l]
            chain_copy(l).start()

        @pl.loop(0, 2 * mine)
        def _(i):
            scores = lax.dot_general(qf[i], kf[i], (((1,), (1,)), ((), ())), preferred_element_type=f32)
            r = lax.broadcasted_iota(jnp.int32, (tokens, tokens), 0)
            c = lax.broadcasted_iota(jnp.int32, (tokens, tokens), 1)
            masked = jnp.where(r >= c, scores, 0.0)
            den[i] = jnp.broadcast_to(jnp.sum(masked, axis=-1, keepdims=True), (tokens, head))
            num[i] = jnp.dot(masked.astype(bf16), vf[i], preferred_element_type=f32)

        kinds = (0,) if split else (0, 1)
        if last:
            @pl.when(jnp.logical_not(held_back))
            def _():
                far(l, 1)

        @pl.when(line == 0)
        def _():
            for h in range(mine):
                prefix[h] = jnp.zeros_like(prefix[h])

        @pl.when(below & (core == 1))
        def _():
            chain_copy(l).wait_recv()
            give_copy(l).start()
            for h in range(mine):
                prefix[h] = st_in[l, 1, h].astype(f32)

        @pl.when(below & above & (core == 1))
        def _():
            state_copy(l).wait_recv()
            for h in range(mine):
                st_out[l, 0, h] = (st_in[l, 0, h].astype(f32) + st_held[l, h].astype(f32)).astype(bf16)
                st_out[l, 1, h] = (prefix[h] + own_state[2 * h] + own_state[2 * h + 1]).astype(bf16)
            chain_copy(l).start()

        if not last:
            @pl.when(held_back)
            def _():
                z_up(start, l + 1, *early)
        else:
            @pl.when(held_back)
            def _():
                far(l, 1)

        @pl.when(below & (core == 0))
        def _():
            give_copy(l).wait_recv()
            for h in range(mine):
                prefix[h] = st_give[l, h].astype(f32)

        @pl.loop(0, 2 * mine)
        def _(i):
            h, b = i // 2, i % 2
            before = prefix[h] + own_state[2 * h] * jnp.where(b == 1, 1.0, 0.0)
            q = qf[i]
            d = den[i] + jnp.sum(q.astype(f32) * before[feats : feats + 1], axis=-1, keepdims=True)
            n = num[i] + jnp.dot(q, before[:feats].astype(bf16), preferred_element_type=f32)
            a = n / d
            norm = lax.rsqrt(jnp.mean(a * a, axis=-1, keepdims=True) + 1e-06)
            to_rows = pl.ds(pl.multiple_of(b * tokens, tokens), tokens)
            to_cols = pl.ds(pl.multiple_of(h * head, 128), head)
            to_gain = pl.ds(pl.multiple_of((parity * mine + h) * head, 128), head)
            att[to_rows, to_cols] = (a * norm * out_gain[l : l + 1, to_gain]).astype(bf16)

        weights_wait(l, 1)
        per = width // oc

        def project(p, g):
            a = att[pl.ds(pl.multiple_of(p * tokens, tokens), tokens), :]
            for i in range(per):
                part[p, g, :, i * oc : (i + 1) * oc] = jnp.dot(
                    a, wo[l, g * per + i], preferred_element_type=f32
                ).astype(bf16)

        @pl.loop(0, 2 * chips)
        def _(n):
            p = lax.rem(other + n // chips, 2)
            x = lax.rem(chip + 1 + n % chips, chips)
            project(p, x * 2 + 1 - core)
            d_copy(l, p, x).start()

        @pl.loop(0, 2 * chips)
        def _(n):
            p = lax.rem(other + n // chips, 2)
            x = lax.rem(chip + 1 + n % chips, chips)
            project(p, x * 2 + core)

        if not last:
            inward(l + 1, *kinds)
        hops = list(range(1, chips)) + [0]
        for own in range(2):
            p = parity if own else other
            for j in hops:
                x = chip_at(j)
                d_copy(l, p, x).wait_recv()

                @pl.loop(0, tokens // step_rows)
                def _(t, p=p, x=x, j=j):
                    at = pl.ds(pl.multiple_of(t * step_rows, step_rows), step_rows)
                    part[p, beside(j), at, :] = (
                        part[p, beside(j), at, :].astype(f32) + rsd[p, x, at, :].astype(f32)
                    ).astype(bf16)

                if j:
                    x_copy(l, p, j).start()
                if not own:
                    w_copy(l, j).start()

        if last:
            for n in range(l):
                drain(n)
        else:
            outward(l + 1, *kinds)
        for j in range(1, chips):
            x_arrival(l, other, j).wait_recv()

        @pl.loop(0, half // step_rows)
        def _(t):
            at = pl.ds(pl.multiple_of(t * step_rows, step_rows), step_rows)
            total = part[other, grp, at, :].astype(f32)
            for j in range(1, chips):
                total = total + rx[other, chip_at(j), at, :].astype(f32)
            ub[at, :] = total.astype(bf16)

        u_copy(l).start()
        for j in hops:
            w_arrival = remote(ry.at[chip_at(j)], ry.at[chip_at(j)], w_send.at[j], w_recv.at[chip_at(j)], to_pair)
            w_arrival.wait_recv()
            if j:
                @pl.loop(0, half // step_rows)
                def _(t, j=j):
                    at = pl.ds(pl.multiple_of(t * step_rows, step_rows), step_rows)
                    low = pl.ds(pl.multiple_of(half + t * step_rows, step_rows), step_rows)
                    vb[chip_at(j), at, :] = (
                        part[parity, beside(j), low, :].astype(f32) + ry[chip_at(j), at, :].astype(f32)
                    ).astype(bf16)

                v_copy(l, j).start()
        if last:
            drain(l)
        for j in range(1, chips):
            x_arrival(l, parity, j).wait_recv()
        u_copy(l).wait_recv()

        def finish(at, total):
            xg[parity, grp, at, :] = (xg[parity, grp, at, :].astype(f32) + total).astype(bf16)

        def result(h):
            return pltpu.make_async_copy(xg.at[parity, grp, piece(h)], out.at[piece(h)], local_sem.at[2 + 2 * layers + h])

        @pl.loop(0, half // step_rows)
        def _(t):
            at = pl.ds(pl.multiple_of(t * step_rows, step_rows), step_rows)
            total = part[parity, grp, at, :].astype(f32) + ru[at, :].astype(f32)
            for j in range(1, chips):
                total = total + rx[parity, chip_at(j), at, :].astype(f32)
            finish(at, total)

        if last:
            result(0).start()
        for j in range(1, chips):
            v_arrival(l, j).wait_recv()

        @pl.loop(0, half // step_rows)
        def _(t):
            at = pl.ds(pl.multiple_of(t * step_rows, step_rows), step_rows)
            low = pl.ds(pl.multiple_of(half + t * step_rows, step_rows), step_rows)
            total = part[parity, grp, low, :].astype(f32) + ry[chip, at, :].astype(f32)
            for j in range(1, chips):
                total = total + rv[chip_at(j), at, :].astype(f32)
            finish(low, total)

        if last:
            result(1).start()
        else:
            ag_start(l + 1)
            far(l + 1, *kinds)
            if split:
                z_start(l + 1, 1)
        for p in range(2):
            for x in range(chips):
                d_copy(l, p, x).wait_send()
            for j in range(1, chips):
                x_copy(l, p, j).wait_send()
        for j in range(chips):
            w_copy(l, j).wait_send()
        u_copy(l).wait_send()
        for j in range(1, chips):
            v_copy(l, j).wait_send()
        if last:
            for h in range(2):
                result(h).wait()


def local(n_seq, n_grp, hidden, qkv_weight, out_weight, projection, norm_gain, out_gain):
    layers, rows, cols = qkv_weight.shape
    depth, oc = out_weight.shape[1:]
    heads, head, feats = projection.shape[1:]
    tokens, width = hidden.shape
    lines, chips, mine, half = n_seq // 2, n_grp // 2, heads // 2, tokens // 2
    dma = pltpu.SemaphoreType.DMA
    vmem = pl.BlockSpec(memory_space=pltpu.VMEM)
    anywhere = pl.BlockSpec(memory_space=pl.ANY)
    state = (feats + 16, head)
    return pl.pallas_call(
        functools.partial(kernel, n_seq, n_grp),
        out_shape=jax.ShapeDtypeStruct((tokens, width), bf16),
        in_specs=[anywhere, anywhere, anywhere, anywhere, vmem, vmem],
        out_specs=anywhere,
        scratch_shapes=[
            pltpu.VMEM((layers, n_seq, rows, cols // 2), bf16),
            pltpu.VMEM((layers, n_seq, depth // 2, oc), bf16),
            pltpu.VMEM((2, n_grp, tokens, width), bf16),
            pltpu.VMEM((2, n_grp, tokens, width), bf16),
            pltpu.VMEM((2, chips, tokens, width), bf16),
            pltpu.VMEM((2, chips, half, width), bf16),
            pltpu.VMEM((chips, half, width), bf16),
            pltpu.VMEM((chips, half, width), bf16),
            pltpu.VMEM((half, width), bf16),
            pltpu.VMEM((half, width), bf16),
            pltpu.VMEM((chips, half, width), bf16),
            pltpu.VMEM((2 * tokens, n_grp * width), bf16),
            pltpu.VMEM((heads, tokens, feats), bf16),
            pltpu.VMEM((heads, tokens, feats), bf16),
            pltpu.VMEM((heads, tokens, head), bf16),
            pltpu.VMEM((heads, tokens, head), f32),
            pltpu.VMEM((heads, tokens, head), f32),
            pltpu.VMEM((2 * tokens, mine * head), bf16),
            pltpu.VMEM((layers, mine, head, feats), f32),
            pltpu.VMEM((layers, mine, head, 3 * feats), bf16),
            pltpu.VMEM((heads,) + state, f32),
            pltpu.VMEM((layers, mine) + state, bf16),
            pltpu.VMEM((layers, mine) + state, bf16),
            pltpu.VMEM((layers, 2, mine) + state, bf16),
            pltpu.VMEM((layers, 2, mine) + state, bf16),
            pltpu.VMEM((layers, mine) + state, bf16),
            pltpu.VMEM((mine,) + state, f32),
            dma((4 + 2 * layers,)),
            dma((layers, 2, 2)),
            dma((layers, 2, lines)),
            dma((layers, 2, lines)),
            dma((layers, 2)),
            dma((layers, 2)),
            dma((layers,)),
            dma((layers,)),
            dma((layers,)),
            dma((layers,)),
            dma((layers,)),
            dma((layers,)),
            dma((8 * chips - 2,)),
            dma((2, n_grp, 2)),
            dma((2, chips)),
            dma((2, chips)),
            dma((2, chips)),
            dma((2, chips)),
            dma((chips,)),
            dma((chips,)),
            dma((1,)),
            dma((1,)),
            dma((chips,)),
            dma((chips,)),
        ],
        compiler_params=pltpu.CompilerParams(
            collective_id=0, has_side_effects=True, vmem_limit_bytes=66_000_000
        ),
    )(hidden, qkv_weight, out_weight, projection, norm_gain, out_gain)


def solution(mesh):
    return jax.shard_map(
        functools.partial(local, mesh.shape["seq"], mesh.shape["grp"]),
        mesh=mesh,
        in_specs=(
            P("seq", "grp"),
            P(None, "seq", "grp"),
            P(None, "grp", "seq"),
            P(None, "grp", None, None),
            P(),
            P(None, "grp"),
        ),
        out_specs=P("seq", "grp"),
        check_vma=False,
    )
```

```python
import functools
import math

import jax
import jax.numpy as jnp
from jax import lax
from jax.experimental import pallas as pl
from jax.experimental.pallas import tpu as pltpu
from jax.sharding import PartitionSpec as P

MESH = pl.DeviceIdType.MESH
stabilizer = 2.0
f32 = jnp.float32
bf16 = jnp.bfloat16


def remote(src, dst, send, recv, device):
    return pltpu.make_async_remote_copy(
        src_ref=src, dst_ref=dst, send_sem=send, recv_sem=recv, device_id=device, device_id_type=MESH
    )


def kernel(
    n_seq, n_grp, hidden, qkv_w, out_w, proj, norm_gain, out_gain, out,
    wq, wo, xg, part, rsd, rx, ry, rv, ru, ub, vb, normed, qf, kf, vf, num, den, att,
    proj_f, terms, own_state, st_send, st_held, st_in, st_out, st_give, prefix,
    local_sem, z_send, z_recv, r_send, y_send, y_recv, l_send, l_recv, m_send, m_recv, k_send, k_recv,
    ag_send, ag_recv, d_send, d_recv, x_send, x_recv, w_send, w_recv, u_send, u_recv, v_send, v_recv,
):
    layers, rows, cols = qkv_w.shape
    depth, oc = out_w.shape[1:]
    tokens, width = hidden.shape
    heads, head = proj.shape[1:3]
    feats = proj.shape[3]
    lines = n_seq // 2
    chips = n_grp // 2
    mine = heads // 2
    half = tokens // 2
    step_rows = 64
    me = lax.axis_index("seq")
    grp = lax.axis_index("grp")
    line, parity = me // 2, me % 2
    other = 1 - parity
    pair = line * 2 + other
    chip, core = grp // 2, grp % 2
    partner = chip * 2 + 1 - core

    def chip_at(j):
        return lax.rem(chip + j, chips)

    def beside(j):
        return chip_at(j) * 2 + core

    def piece(h):
        return pl.ds(h * half, half)

    def weight(l, k, slot):
        return (wo if k else wq).at[l, slot]

    def line_pair(l, k, where):
        return (wo if k else wq).at[l, pl.ds(where * 2, 2)]

    def own_part(l, k, who):
        if k:
            return out_w.at[l, pl.ds(pl.multiple_of(who * (depth // 2), depth // 2), depth // 2)]
        return qkv_w.at[l, :, pl.ds(pl.multiple_of(who * (cols // 2), cols // 2), cols // 2)]

    own_copies = [
        [pltpu.make_async_copy(own_part(l, k, parity), weight(l, k, me), local_sem.at[1 + 2 * l + k]) for k in range(2)]
        for l in range(layers)
    ]
    own_hidden = pltpu.make_async_copy(hidden, xg.at[parity, grp], local_sem.at[0])
    for pieces in own_copies:
        for c in pieces:
            c.start()
    own_hidden.start()
    own_proj = pltpu.make_async_copy(proj.at[:, pl.ds(parity * mine, mine)], proj_f, local_sem.at[1 + 2 * layers])
    own_proj.start()

    barrier = pltpu.get_barrier_semaphore()
    for k in range(1, lines):
        pl.semaphore_signal(barrier, inc=1, device_id={"seq": lax.rem(line + k, lines) * 2 + parity}, device_id_type=MESH)
    pl.semaphore_signal(barrier, inc=1, device_id={"seq": pair}, device_id_type=MESH)
    for k in range(1, n_grp):
        pl.semaphore_signal(barrier, inc=1, device_id={"grp": lax.rem(grp + k, n_grp)}, device_id_type=MESH)
    pl.semaphore_wait(barrier, lines + n_grp - 1)

    def slot_of(where, side):
        return where * 2 + (other if side else parity)

    def y_copy(l, k):
        return remote(own_part(l, k, other), weight(l, k, me), y_send.at[l, k], y_recv.at[l, k], {"seq": pair})

    def y_arrival(l, k):
        return remote(weight(l, k, pair), weight(l, k, pair), y_send.at[l, k], y_recv.at[l, k], {"seq": pair})

    def z_copy(l, k, way, side=None):
        ref = line_pair(l, k, line) if side is None else weight(l, k, slot_of(line, side))
        to = line - 1 if way else line + 1
        return remote(ref, ref, z_send.at[l, k, way], z_recv.at[l, k, line], {"seq": to * 2 + parity})

    def z_arrival(l, k, src):
        ref = line_pair(l, k, src)
        return remote(ref, ref, z_send.at[l, k, 0], z_recv.at[l, k, src], {"seq": pair})

    def r_copy(l, k, src, way):
        ref = line_pair(l, k, src)
        to = line - 1 if way else line + 1
        return remote(ref, ref, r_send.at[l, k, src], z_recv.at[l, k, src], {"seq": to * 2 + parity})

    def span(count, body):
        if count <= 4:
            for t in range(count):
                body(t)
        else:
            pl.loop(0, count)(body)

    def z_up(act, l, *kinds, side=None):
        @pl.when(line + 1 < lines)
        def _():
            for k in kinds:
                act(z_copy(l, k, 0, side))

    def z_down(act, l, *kinds, side=None):
        @pl.when(line >= 1)
        def _():
            for k in kinds:
                act(z_copy(l, k, 1, side))

    def start(c):
        c.start()

    def z_start(l, *kinds, side=None):
        z_up(start, l, *kinds, side=side)
        z_down(start, l, *kinds, side=side)

    upper = 2 * line >= lines

    def r_each(hop, act, where=None):
        up, down = (line >= hop) & (line + 1 < lines), (line + hop < lines) & (line >= 1)
        if where is not None:
            up, down = up & (upper == where), down & (upper != where)

        @pl.when(up)
        def _():
            act(line - hop, 0)

        @pl.when(down)
        def _():
            act(line + hop, 1)

    def forward(l, k, hop, where=None):
        def act(src, way):
            z_arrival(l, k, src).wait_recv()
            r_copy(l, k, src, way).start()

        r_each(hop, act, where)

    def outward(l, *kinds):
        for k in kinds:
            forward(l, k, 1, True)

    def inward(l, *kinds):
        for k in kinds:
            forward(l, k, 1, False)

    def far(l, *kinds):
        for k in kinds:
            span(lines - 3, lambda t: forward(l, k, t + 2))

    def weights_wait(l, k):
        def body(src):
            @pl.when((src != line) & ((line == 0) | (line == lines - 1)))
            def _():
                z_arrival(l, k, src).wait_recv()

        span(lines, body)

    def prepare(l):
        for c in own_copies[l]:
            c.wait()
        for k in range(2):
            y_arrival(l, k).wait_recv()

    def ag_copy(l, p, g, h, place, device):
        ref = xg.at[p, g, piece(h)]
        return remote(ref, ref, ag_send.at[place], ag_recv.at[p, g, h], device)

    to_pair, to_partner = {"seq": pair}, {"grp": partner}

    def ag_wait(l, p, g, h):
        ag_copy(l, p, g, h, 0, to_pair).wait_recv()

    def ag_sends(l):
        across = [{"grp": beside(j)} for j in range(1, chips)]
        own = [(1, d) for d in across] + [(0, to_pair)] + [(0, d) for d in across] + [(1, to_pair)]
        own += [(h, to_partner) for h in range(2)]
        passed = [((other, grp, 0), across)]
        passed += [((parity, beside(j), 1), [to_pair]) for j in range(1, chips)]
        passed += [((other, grp, 1), [])] + [((parity, beside(j), 0), []) for j in range(1, chips)]
        passed += [((other, beside(j), h), []) for j in range(1, chips) for h in range(2)]
        first = [(parity, grp, h, n, d) for n, (h, d) in enumerate(own)]
        second, n = [], len(first)
        for slot, targets in passed:
            second.append((slot, [slot + (n + i, d) for i, d in enumerate(targets + [to_partner])]))
            n += len(targets) + 1
        return first, second

    def ag_start(l):
        for args in ag_sends(l)[0]:
            ag_copy(l, *args).start()

    def ag_own(l):
        for slot, targets in ag_sends(l)[1][: 2 * chips]:
            ag_pass(l, slot, targets)
        ag_beside(l, parity)

    def ag_other(l):
        for slot, targets in ag_sends(l)[1][2 * chips :]:
            ag_pass(l, slot, targets)
        ag_beside(l, other)

    def ag_pass(l, slot, targets):
        ag_wait(l, *slot)
        for args in targets:
            ag_copy(l, *args).start()

    def ag_beside(l, p):
        for h in range(2):
            ag_wait(l, p, partner, h)
            for j in range(1, chips):
                ag_wait(l, p, chip_at(j) * 2 + 1 - core, h)

    def ag_drain(l):
        first, second = ag_sends(l)
        for args in first + [a for _, targets in second for a in targets]:
            ag_copy(l, *args).wait_send()

    def d_copy(l, p, x):
        return remote(part.at[p, x * 2 + 1 - core], rsd.at[p, x], d_send.at[p, x], d_recv.at[p, x], to_partner)

    def x_copy(l, p, j):
        return remote(
            part.at[p, beside(j), piece(0)], rx.at[p, chip], x_send.at[p, j], x_recv.at[p, chip], {"grp": beside(j)}
        )

    def x_arrival(l, p, j):
        ref = rx.at[p, chip_at(j)]
        return remote(ref, ref, x_send.at[p, j], x_recv.at[p, chip_at(j)], {"grp": beside(j)})

    def w_copy(l, j):
        x = chip_at(j)
        return remote(part.at[other, beside(j), piece(1)], ry.at[x], w_send.at[x], w_recv.at[x], to_pair)

    def u_copy(l):
        return remote(ub, ru, u_send.at[0], u_recv.at[0], to_pair)

    def v_copy(l, j):
        return remote(vb.at[chip_at(j)], rv.at[chip], v_send.at[j], v_recv.at[chip], {"grp": beside(j)})

    def v_arrival(l, j):
        ref = rv.at[chip_at(j)]
        return remote(ref, ref, v_send.at[j], v_recv.at[chip_at(j)], {"grp": beside(j)})

    def state_copy(l):
        return remote(st_send.at[l], st_held.at[l], k_send.at[l], k_recv.at[l], to_partner)

    def chain_copy(l):
        return remote(st_out.at[l], st_in.at[l], l_send.at[l], l_recv.at[l], {"seq": line * 2 + 2 + parity})

    def give_copy(l):
        return remote(st_in.at[l, 0], st_give.at[l], m_send.at[l], m_recv.at[l], to_partner)

    below, above = line >= 1, line + 1 < lines
    held_back = (core == 1) & (line == lines - 2)

    def wait_send(c):
        c.wait_send()

    def drain(l):
        for k in range(2):
            y_copy(l, k).wait_send()
            z_up(wait_send, l, k)
            z_down(wait_send, l, k)

            def forwarded(t, k=k):
                r_each(t + 1, lambda src, way: r_copy(l, k, src, way).wait_send())

            span(lines - 2, forwarded)

        @pl.when(above & (core == 0))
        def _():
            state_copy(l).wait_send()

        @pl.when(above & (core == 1))
        def _():
            chain_copy(l).wait_send()

        @pl.when(below & (core == 1))
        def _():
            give_copy(l).wait_send()

    for k in range(2):
        y_copy(0, k).start()
    for c in own_copies[0]:
        c.wait()
    z_start(0, 0, side=0)
    z_start(0, 1, side=0)
    own_hidden.wait()
    ag_start(0)
    if layers > 1:
        for k in range(2):
            y_copy(1, k).start()
    y_arrival(0, 0).wait_recv()
    z_start(0, 0, side=1)
    y_arrival(0, 1).wait_recv()
    z_start(0, 1, side=1)
    for k in range(2):
        outward(0, k)
        inward(0, k)

    scale = head ** (-0.25)
    inv = 1.0 / math.sqrt(feats)

    def features(u, terms):
        mixed = jnp.dot(u, terms, preferred_element_type=f32)
        mixed = (mixed[:, 2 * feats :] + mixed[:, feats : 2 * feats]) + mixed[:, :feats]
        w0 = u.astype(f32) * scale
        energy = 0.5 * jnp.sum(w0 * w0, axis=-1, keepdims=True)
        return (jnp.exp(mixed - energy - stabilizer) * inv).astype(bf16)

    for l in range(layers):
        last = l == layers - 1
        def normalize(b):
            @pl.loop(0, tokens // step_rows)
            def _(t):
                at = pl.ds(pl.multiple_of(b * tokens + t * step_rows, step_rows), step_rows)
                src = pl.ds(pl.multiple_of(t * step_rows, step_rows), step_rows)
                wide = [xg[b, g, src, :].astype(f32) for g in range(n_grp)]
                total = sum(jnp.sum(v * v, axis=-1, keepdims=True) for v in wide)
                rms = lax.rsqrt(total / (width * n_grp) + 1e-05)
                for g in range(n_grp):
                    cut = slice(g * width, (g + 1) * width)
                    normed[at, cut] = (wide[g] * rms * norm_gain[l : l + 1, cut]).astype(bf16)

        ag_own(l)
        normalize(parity)
        ag_other(l)
        if l == 0:
            for n in range(2, layers):
                for k in range(2):
                    y_copy(n, k).start()
        elif last:
            outward(l, 1)
            inward(l, 1)
        normalize(other)
        ag_drain(l)
        if l == 0:
            far(0, 0, 1)
        split = l + 1 == layers - 1
        early = (0,) if split else (0, 1)
        if not last:
            prepare(l + 1)
            z_down(start, l + 1, *early)

            @pl.when(jnp.logical_not(held_back))
            def _():
                z_up(start, l + 1, *early)

        if l == 0:
            own_proj.wait()

            @pl.loop(0, layers * mine)
            def _(i):
                n, h = i // mine, i % mine
                scaled = proj_f[n, h] * scale
                high = scaled.astype(bf16)
                rest = scaled - high.astype(f32)
                mid = rest.astype(bf16)
                terms[n, h, :, :feats] = high
                terms[n, h, :, feats : 2 * feats] = mid
                terms[n, h, :, 2 * feats :] = (rest - mid.astype(f32)).astype(bf16)

        weights_wait(l, 0)

        @pl.loop(0, 2 * mine)
        def _(i):
            h, b = i // 2, i % 2
            at = pl.ds(pl.multiple_of(h * 3 * head, 128), 3 * head)
            w = wq[l, :, :, at].reshape(n_seq * rows, 3 * head)
            x = normed[pl.ds(pl.multiple_of(b * tokens, tokens), tokens), :]
            qkv = jnp.dot(x, w, preferred_element_type=f32).astype(bf16)
            split_terms = terms[l, h]
            key = features(qkv[:, head : 2 * head], split_terms)
            value = qkv[:, 2 * head :]
            qf[i] = features(qkv[:, :head], split_terms)
            kf[i] = key
            vf[i] = value
            own_state[i, :feats] = lax.dot_general(key, value, (((0,), (0,)), ((), ())), preferred_element_type=f32)
            own_state[i, feats:] = jnp.dot(jnp.ones((16, tokens), bf16), key, preferred_element_type=f32)

        for h in range(mine):
            st_send[l, h] = (own_state[2 * h] + own_state[2 * h + 1]).astype(bf16)

        @pl.when(above & (core == 0))
        def _():
            state_copy(l).start()

        @pl.when(above & (core == 1) & (line == 0))
        def _():
            state_copy(l).wait_recv()
            st_out[l, 0] = st_held[l]
            st_out[l, 1] = st_send[l]
            chain_copy(l).start()

        @pl.loop(0, 2 * mine)
        def _(i):
            scores = lax.dot_general(qf[i], kf[i], (((1,), (1,)), ((), ())), preferred_element_type=f32)
            r = lax.broadcasted_iota(jnp.int32, (tokens, tokens), 0)
            c = lax.broadcasted_iota(jnp.int32, (tokens, tokens), 1)
            masked = jnp.where(r >= c, scores, 0.0)
            den[i] = jnp.broadcast_to(jnp.sum(masked, axis=-1, keepdims=True), (tokens, head))
            num[i] = jnp.dot(masked.astype(bf16), vf[i], preferred_element_type=f32)

        kinds = (0,) if split else (0, 1)
        if last:
            @pl.when(jnp.logical_not(held_back))
            def _():
                far(l, 1)

        @pl.when(line == 0)
        def _():
            for h in range(mine):
                prefix[h] = jnp.zeros_like(prefix[h])

        @pl.when(below & (core == 1))
        def _():
            chain_copy(l).wait_recv()
            give_copy(l).start()
            for h in range(mine):
                prefix[h] = st_in[l, 1, h].astype(f32)

        @pl.when(below & above & (core == 1))
        def _():
            state_copy(l).wait_recv()
            for h in range(mine):
                st_out[l, 0, h] = (st_in[l, 0, h].astype(f32) + st_held[l, h].astype(f32)).astype(bf16)
                st_out[l, 1, h] = (prefix[h] + own_state[2 * h] + own_state[2 * h + 1]).astype(bf16)
            chain_copy(l).start()

        if not last:
            @pl.when(held_back)
            def _():
                z_up(start, l + 1, *early)
        else:
            @pl.when(held_back)
            def _():
                far(l, 1)

        @pl.when(below & (core == 0))
        def _():
            give_copy(l).wait_recv()
            for h in range(mine):
                prefix[h] = st_give[l, h].astype(f32)

        @pl.loop(0, 2 * mine)
        def _(i):
            h, b = i // 2, i % 2
            before = prefix[h] + own_state[2 * h] * jnp.where(b == 1, 1.0, 0.0)
            q = qf[i]
            d = den[i] + jnp.sum(q.astype(f32) * before[feats : feats + 1], axis=-1, keepdims=True)
            n = num[i] + jnp.dot(q, before[:feats].astype(bf16), preferred_element_type=f32)
            a = n / d
            norm = lax.rsqrt(jnp.mean(a * a, axis=-1, keepdims=True) + 1e-06)
            to_rows = pl.ds(pl.multiple_of(b * tokens, tokens), tokens)
            to_cols = pl.ds(pl.multiple_of(h * head, 128), head)
            to_gain = pl.ds(pl.multiple_of((parity * mine + h) * head, 128), head)
            att[to_rows, to_cols] = (a * norm * out_gain[l : l + 1, to_gain]).astype(bf16)

        weights_wait(l, 1)
        per = width // oc

        def project(p, g):
            a = att[pl.ds(pl.multiple_of(p * tokens, tokens), tokens), :]
            for i in range(per):
                part[p, g, :, i * oc : (i + 1) * oc] = jnp.dot(
                    a, wo[l, g * per + i], preferred_element_type=f32
                ).astype(bf16)

        if not last:
            inward(l + 1, *kinds)
        hops = list(range(1, chips)) + [0]

        def make(p, j):
            x = chip_at(j)
            project(p, x * 2 + 1 - core)
            d_copy(l, p, x).start()
            project(p, beside(j))

        def combine(p, j, onward):
            x = chip_at(j)
            d_copy(l, p, x).wait_recv()

            @pl.loop(0, tokens // step_rows)
            def _(t):
                at = pl.ds(pl.multiple_of(t * step_rows, step_rows), step_rows)
                part[p, beside(j), at, :] = (
                    part[p, beside(j), at, :].astype(f32) + rsd[p, x, at, :].astype(f32)
                ).astype(bf16)

            if j:
                x_copy(l, p, j).start()
            if onward:
                w_copy(l, j).start()

        todo = [(other, j, True) for j in hops] + [(parity, j, False) for j in hops]
        ahead = 2
        for n, (p, j, onward) in enumerate(todo):
            make(p, j)
            if n + 1 >= ahead:
                combine(*todo[n + 1 - ahead])
        for n in range(len(todo) + 1 - ahead, len(todo)):
            combine(*todo[n])
        if last:
            for n in range(l):
                drain(n)
        else:
            outward(l + 1, *kinds)
        for j in range(1, chips):
            x_arrival(l, other, j).wait_recv()

        @pl.loop(0, half // step_rows)
        def _(t):
            at = pl.ds(pl.multiple_of(t * step_rows, step_rows), step_rows)
            total = part[other, grp, at, :].astype(f32)
            for j in range(1, chips):
                total = total + rx[other, chip_at(j), at, :].astype(f32)
            ub[at, :] = total.astype(bf16)

        u_copy(l).start()
        for j in hops:
            w_arrival = remote(ry.at[chip_at(j)], ry.at[chip_at(j)], w_send.at[j], w_recv.at[chip_at(j)], to_pair)
            w_arrival.wait_recv()
            if j:
                @pl.loop(0, half // step_rows)
                def _(t, j=j):
                    at = pl.ds(pl.multiple_of(t * step_rows, step_rows), step_rows)
                    low = pl.ds(pl.multiple_of(half + t * step_rows, step_rows), step_rows)
                    vb[chip_at(j), at, :] = (
                        part[parity, beside(j), low, :].astype(f32) + ry[chip_at(j), at, :].astype(f32)
                    ).astype(bf16)

                v_copy(l, j).start()
        if last:
            drain(l)
        for j in range(1, chips):
            x_arrival(l, parity, j).wait_recv()
        u_copy(l).wait_recv()

        def finish(at, total):
            xg[parity, grp, at, :] = (xg[parity, grp, at, :].astype(f32) + total).astype(bf16)

        def result(h):
            return pltpu.make_async_copy(xg.at[parity, grp, piece(h)], out.at[piece(h)], local_sem.at[2 + 2 * layers + h])

        @pl.loop(0, half // step_rows)
        def _(t):
            at = pl.ds(pl.multiple_of(t * step_rows, step_rows), step_rows)
            total = part[parity, grp, at, :].astype(f32) + ru[at, :].astype(f32)
            for j in range(1, chips):
                total = total + rx[parity, chip_at(j), at, :].astype(f32)
            finish(at, total)

        if last:
            result(0).start()
        for j in range(1, chips):
            v_arrival(l, j).wait_recv()

        @pl.loop(0, half // step_rows)
        def _(t):
            at = pl.ds(pl.multiple_of(t * step_rows, step_rows), step_rows)
            low = pl.ds(pl.multiple_of(half + t * step_rows, step_rows), step_rows)
            total = part[parity, grp, low, :].astype(f32) + ry[chip, at, :].astype(f32)
            for j in range(1, chips):
                total = total + rv[chip_at(j), at, :].astype(f32)
            finish(low, total)

        if last:
            result(1).start()
        else:
            ag_start(l + 1)
            far(l + 1, *kinds)
            if split:
                z_start(l + 1, 1)
        for p in range(2):
            for x in range(chips):
                d_copy(l, p, x).wait_send()
            for j in range(1, chips):
                x_copy(l, p, j).wait_send()
        for j in range(chips):
            w_copy(l, j).wait_send()
        u_copy(l).wait_send()
        for j in range(1, chips):
            v_copy(l, j).wait_send()
        if last:
            for h in range(2):
                result(h).wait()


def local(n_seq, n_grp, hidden, qkv_weight, out_weight, projection, norm_gain, out_gain):
    layers, rows, cols = qkv_weight.shape
    depth, oc = out_weight.shape[1:]
    heads, head, feats = projection.shape[1:]
    tokens, width = hidden.shape
    lines, chips, mine, half = n_seq // 2, n_grp // 2, heads // 2, tokens // 2
    dma = pltpu.SemaphoreType.DMA
    vmem = pl.BlockSpec(memory_space=pltpu.VMEM)
    anywhere = pl.BlockSpec(memory_space=pl.ANY)
    state = (feats + 16, head)
    return pl.pallas_call(
        functools.partial(kernel, n_seq, n_grp),
        out_shape=jax.ShapeDtypeStruct((tokens, width), bf16),
        in_specs=[anywhere, anywhere, anywhere, anywhere, vmem, vmem],
        out_specs=anywhere,
        scratch_shapes=[
            pltpu.VMEM((layers, n_seq, rows, cols // 2), bf16),
            pltpu.VMEM((layers, n_seq, depth // 2, oc), bf16),
            pltpu.VMEM((2, n_grp, tokens, width), bf16),
            pltpu.VMEM((2, n_grp, tokens, width), bf16),
            pltpu.VMEM((2, chips, tokens, width), bf16),
            pltpu.VMEM((2, chips, half, width), bf16),
            pltpu.VMEM((chips, half, width), bf16),
            pltpu.VMEM((chips, half, width), bf16),
            pltpu.VMEM((half, width), bf16),
            pltpu.VMEM((half, width), bf16),
            pltpu.VMEM((chips, half, width), bf16),
            pltpu.VMEM((2 * tokens, n_grp * width), bf16),
            pltpu.VMEM((heads, tokens, feats), bf16),
            pltpu.VMEM((heads, tokens, feats), bf16),
            pltpu.VMEM((heads, tokens, head), bf16),
            pltpu.VMEM((heads, tokens, head), f32),
            pltpu.VMEM((heads, tokens, head), f32),
            pltpu.VMEM((2 * tokens, mine * head), bf16),
            pltpu.VMEM((layers, mine, head, feats), f32),
            pltpu.VMEM((layers, mine, head, 3 * feats), bf16),
            pltpu.VMEM((heads,) + state, f32),
            pltpu.VMEM((layers, mine) + state, bf16),
            pltpu.VMEM((layers, mine) + state, bf16),
            pltpu.VMEM((layers, 2, mine) + state, bf16),
            pltpu.VMEM((layers, 2, mine) + state, bf16),
            pltpu.VMEM((layers, mine) + state, bf16),
            pltpu.VMEM((mine,) + state, f32),
            dma((4 + 2 * layers,)),
            dma((layers, 2, 2)),
            dma((layers, 2, lines)),
            dma((layers, 2, lines)),
            dma((layers, 2)),
            dma((layers, 2)),
            dma((layers,)),
            dma((layers,)),
            dma((layers,)),
            dma((layers,)),
            dma((layers,)),
            dma((layers,)),
            dma((8 * chips - 2,)),
            dma((2, n_grp, 2)),
            dma((2, chips)),
            dma((2, chips)),
            dma((2, chips)),
            dma((2, chips)),
            dma((chips,)),
            dma((chips,)),
            dma((1,)),
            dma((1,)),
            dma((chips,)),
            dma((chips,)),
        ],
        compiler_params=pltpu.CompilerParams(
            collective_id=0, has_side_effects=True, vmem_limit_bytes=66_000_000
        ),
    )(hidden, qkv_weight, out_weight, projection, norm_gain, out_gain)


def solution(mesh):
    return jax.shard_map(
        functools.partial(local, mesh.shape["seq"], mesh.shape["grp"]),
        mesh=mesh,
        in_specs=(
            P("seq", "grp"),
            P(None, "seq", "grp"),
            P(None, "grp", "seq"),
            P(None, "grp", None, None),
            P(),
            P(None, "grp"),
        ),
        out_specs=P("seq", "grp"),
        check_vma=False,
    )
```
